32 devices in a mesh: subj: 16 (over z, y, x), vox: 2 (over core).
Axes of the slice: x: 2, y: 2, z: 4, core: 2. Of those that a mesh axis runs over, the one named last changes fastest.
Arguments:
- bold_series: float32 [16, 300, 16384], P('subj', None, 'vox')
- seed_index: int32 [256], replicated, may hold values from 0 to 16383
Outputs:
- group_z: float32 [16384, 256], P(('vox', 'subj'))
The draws below stay inside these ranges and needn't reach their ends.
All inputs are finite; a program needn't handle non-finite values.
Results may differ from the reference program's by a relative error of at most 0.00031.
Values may be sent and summed in bfloat16 or wider, within the bound.
A program may use at most 64 MiB of HBM per device.

```python
import math
import jax
import jax.numpy as jnp
from jax import lax

TIMEPOINTS = 300
SEEDS = 256
SUBJ = 16
VOXELS = 16384


def draw_bold_series(key, part):
    factors = 4
    subkeys = jax.random.split(key, 6)
    hidden_factors = jax.random.normal(subkeys[0], (SUBJ, factors, TIMEPOINTS), jnp.float32)
    common_component = jax.random.normal(subkeys[1], (factors, VOXELS), jnp.float32) * (0.8 / math.sqrt(factors))
    subject_specific = jax.random.normal(subkeys[2], (SUBJ, factors, VOXELS), jnp.float32) * (0.6 / math.sqrt(factors))
    signal_component = jnp.einsum('oju,ojf->ouf', hidden_factors, common_component[None] + subject_specific)
    noise_part = jax.random.normal(subkeys[3], (SUBJ, TIMEPOINTS, VOXELS), jnp.float32)
    scale_factors = jnp.exp(jax.random.uniform(subkeys[4], (SUBJ, 1, VOXELS), jnp.float32, 0.0, math.log(10.0)))
    offsets = jax.random.uniform(subkeys[5], (SUBJ, 1, VOXELS), jnp.float32, -5.0, 5.0)
    return offsets + scale_factors * (signal_component + noise_part)


def place_ends(drawn, rng, smallest, largest):
    longest = drawn.shape.index(max(drawn.shape))
    spots = []
    for shift in (0, 1):
        where = [jax.random.randint(jax.random.fold_in(rng, axis), (), 0, length) for axis, length in enumerate(drawn.shape)]
        where[longest] = (where[longest] + shift) % drawn.shape[longest]
        spots.append(tuple(where))
    return drawn.at[spots[0]].set(smallest).at[spots[1]].set(largest)


def setup_inputs(seed: int = 0) -> dict:
    arg_keys = jax.random.split(jax.random.key(seed), 3)
    return {
        "bold_series": draw_bold_series(jax.random.fold_in(arg_keys[2], 71), 0),
        "seed_index": place_ends(jax.random.randint(arg_keys[1], (SEEDS,), 0, VOXELS), jax.random.fold_in(arg_keys[1], 1), 0, VOXELS - 1).astype(jnp.int32),
    }


clip_limit = 0.99
epsilon = 1e-05

def normalize(series):
    demean_series = series - lax.optimization_barrier(jnp.mean(series, axis=0, keepdims=True))
    spread = lax.optimization_barrier(jnp.mean(demean_series * demean_series, axis=0, keepdims=True))
    return (demean_series * lax.rsqrt(spread + epsilon)).astype(jnp.bfloat16)

def arctanh_transform(cross_product, length):
    clipped = jnp.clip(cross_product * (1.0 / length), -clip_limit, clip_limit)
    return 0.5 * jnp.log((1.0 + clipped) / (1.0 - clipped))

def reference(bold_series, seed_index):
    length = bold_series.shape[1]

    def accumulate(summed, series):
        normed = normalize(series)
        seed_panel = jnp.take(normed, seed_index.astype(jnp.int32), axis=1)
        cross_product = lax.dot_general(normed, seed_panel, (((0,), (0,)), ((), ())), preferred_element_type=jnp.float32)
        return (summed + arctanh_transform(cross_product, length), None)
    start_sum = jnp.zeros((bold_series.shape[2], seed_index.shape[0]), jnp.float32)
    summed, unused = lax.scan(accumulate, start_sum, bold_series)
    return summed * (1.0 / SUBJ)
```

```python
import functools
import math

import jax
import jax.numpy as jnp
from jax import lax
from jax.experimental import pallas as pl
from jax.experimental.pallas import tpu as pltpu
from jax.sharding import PartitionSpec as P

clip_limit = 0.99
epsilon = 1e-05
MESH = pl.DeviceIdType.MESH
z_limit = 0.5 * math.log((1.0 + clip_limit) / (1.0 - clip_limit))
code_top = 32700.0
pieces = 2
ahead = 2


def encode(value, terms):
    scale = code_top / math.sqrt(terms * z_limit)
    root = value * lax.rsqrt(jnp.maximum(jnp.abs(value), 1e-30))
    return jnp.round(root * scale).astype(jnp.int32).astype(jnp.int16)


def decode(code, terms):
    scale = math.sqrt(terms * z_limit) / code_top
    root = code.astype(jnp.int32).astype(jnp.float32) * scale
    return root * jnp.abs(root)


def kernel(n, nv, chunk, bold, index, result, seeds, out, raw, norm, acc, pan_out, pan_in, pan_t,
           s1_out, s1_in, s2_out, s2_in, s3_out, s3_in,
           load_sem, seed_sem, p_send, p_recv, a_send, a_recv, b_send, b_recv, c_send, c_recv):
    length, columns = norm.shape
    block = columns // n
    hi_count = n // 4
    steps = hi_count * pieces
    width = block // pieces
    offsets = sorted(range(hi_count), key=lambda d: -min(d, hi_count - d))
    s = lax.axis_index("subj")
    v = lax.axis_index("vox")
    odd = lax.rem(v, 2)
    w1, w2 = 1 + odd, 2 - odd
    f, g = lax.rem(s // w1, 2), lax.rem(s // w2, 2)
    hi, lo = s // 4, lax.rem(s, 4)
    mate1 = s + w1 * (1 - 2 * f)
    mate2 = s + w2 * (1 - 2 * g)

    loads, lines = columns // chunk, chunk // 128

    def load(i, j):
        line = i * lines + j
        return pltpu.make_async_copy(bold.at[:, line, :], raw.at[line], load_sem.at[line])

    fetch = pltpu.make_async_copy(index, seeds, seed_sem)
    fetch.start()
    for i in range(loads):
        for j in range(lines):
            load(i, j).start()

    barrier = pltpu.get_barrier_semaphore()
    pl.semaphore_signal(barrier, inc=1, device_id={"subj": mate1}, device_id_type=MESH)
    pl.semaphore_signal(barrier, inc=1, device_id={"subj": mate2}, device_id_type=MESH)
    for j in range(1, hi_count):
        peer = lax.rem(hi + j, hi_count) * 4 + lo
        pl.semaphore_signal(barrier, inc=1, device_id={"subj": peer}, device_id_type=MESH)
    for j in range(1, nv):
        pl.semaphore_signal(
            barrier, inc=1, device_id={"vox": lax.rem(v + j, nv)}, device_id_type=MESH
        )

    acc[...] = jnp.zeros_like(acc)

    def arrive(i):
        for j in range(lines):
            load(i, j).wait()

    def normalize(i):
        for j in range(lines):
            line = i * lines + j
            cols = pl.ds(pl.multiple_of(line * 128, 128), 128)
            x = raw[line]
            x = x - jnp.sum(x, axis=0, keepdims=True) * (1.0 / length)
            spread = jnp.sum(x * x, axis=0, keepdims=True) * (1.0 / length)
            norm[:, cols] = (x * lax.rsqrt(spread + epsilon)).astype(jnp.bfloat16)

    def pick(i):
        cols = pl.ds(pl.multiple_of(i * chunk, 128), chunk)
        rows = lax.broadcasted_iota(jnp.int16, (chunk, seeds.shape[1]), 0)
        place = jnp.clip(seeds[...] - (v * columns + i * chunk), -1, chunk).astype(jnp.int16)
        hit = jnp.where(rows == place, jnp.bfloat16(1.0), jnp.bfloat16(0.0))
        acc[pl.ds(0, length), :] += jnp.dot(
            norm[:, cols], hit, preferred_element_type=jnp.float32,
        )

    fetch.wait()
    arrive(0)
    normalize(0)

    @pl.loop(1, loads)
    def _(i):
        arrive(i)
        pick(i - 1)
        normalize(i)

    pick(loads - 1)

    pl.semaphore_wait(barrier, 2 + (hi_count - 1) + (nv - 1))
    pan_out[...] = acc[pl.ds(0, length), :].astype(jnp.bfloat16)

    def panel_copy(j):
        return pltpu.make_async_remote_copy(
            src_ref=pan_out, dst_ref=pan_in.at[j - 1],
            send_sem=p_send.at[j - 1], recv_sem=p_recv.at[j - 1],
            device_id={"vox": lax.rem(v + j, nv)}, device_id_type=MESH,
        )

    for j in range(1, nv):
        panel_copy(j).start()
    for j in range(1, nv):
        panel_copy(j).wait_recv()
        acc[pl.ds(0, length), :] += pan_in[j - 1].astype(jnp.float32)
    pan_t[...] = acc[...].T.astype(jnp.bfloat16)

    def target_of(step):
        turn = step // pieces
        offset = 0
        for place, d in enumerate(offsets):
            offset = offset + jnp.where(turn == place, d, 0)
        return lax.rem(hi + offset, hi_count)

    def fisher(step, gg, ff):
        start = (target_of(step) * 4 + gg * w2 + ff * w1) * block
        start = start + lax.rem(step, pieces) * width
        cols = pl.ds(pl.multiple_of(start, 128), width)
        cross = jnp.dot(
            pan_t[:, pl.ds(0, length)], norm[:, cols], preferred_element_type=jnp.float32
        )
        c = jnp.clip(cross * (1.0 / length), -clip_limit, clip_limit)
        return 0.5 * (jnp.log(1.0 + c) - jnp.log(1.0 - c))

    def copy1(k):
        return pltpu.make_async_remote_copy(
            src_ref=s1_out.at[k], dst_ref=s1_in.at[k], send_sem=a_send.at[k],
            recv_sem=a_recv.at[k], device_id={"subj": mate1}, device_id_type=MESH,
        )

    def copy2(k):
        return pltpu.make_async_remote_copy(
            src_ref=s2_out.at[k], dst_ref=s2_in.at[k], send_sem=b_send.at[k],
            recv_sem=b_recv.at[k], device_id={"subj": mate2}, device_id_type=MESH,
        )

    def copy3(k):
        target = target_of(k) * 4 + lo
        return pltpu.make_async_remote_copy(
            src_ref=s3_out.at[k], dst_ref=s3_in.at[k], send_sem=c_send.at[k],
            recv_sem=c_recv.at[k], device_id={"subj": target}, device_id_type=MESH,
        )

    @pl.loop(0, steps + ahead + 1)
    def _(turn):
        @pl.when(turn < steps)
        def _():
            s1_out[2 * turn] = encode(fisher(turn, 1 - g, 1 - f), 1)
            copy1(2 * turn).start()
            s1_out[2 * turn + 1] = encode(fisher(turn, g, 1 - f), 1)
            copy1(2 * turn + 1).start()

        @pl.when((turn >= ahead) & (turn < steps + ahead))
        def _():
            k = turn - ahead
            mine = fisher(k, 1 - g, f)
            copy1(2 * k).wait_recv()
            s2_out[k] = encode(mine + decode(s1_in[2 * k], 1), 2)
            copy2(k).start()

        @pl.when(turn >= ahead + 1)
        def _():
            k = turn - ahead - 1
            mine = fisher(k, g, f)
            copy1(2 * k + 1).wait_recv()
            mine = mine + decode(s1_in[2 * k + 1], 1)
            copy2(k).wait_recv()
            mine = mine + decode(s2_in[k], 2)

            @pl.when(k < steps - pieces)
            def _():
                s3_out[k] = encode(mine, 4)
                copy3(k).start()

            @pl.when(k >= steps - pieces)
            def _():
                cols = pl.ds(pl.multiple_of((k - steps + pieces) * width, 128), width)
                out[:, cols] = mine

    for p in range(pieces):
        cols = pl.ds(p * width, width)
        for k in range(p, steps - pieces, pieces):
            copy3(k).wait_recv()
        total = out[:, cols]
        for k in range(p, steps - pieces, pieces):
            total = total + decode(s3_in[k], 4)
        result[cols, :] = (total * (1.0 / n)).T

    for j in range(1, nv):
        panel_copy(j).wait_send()

    @pl.loop(0, 2 * steps)
    def _(k):
        copy1(k).wait_send()

    @pl.loop(0, steps)
    def _(k):
        copy2(k).wait_send()

    @pl.loop(0, steps - pieces)
    def _(k):
        copy3(k).wait_send()


def body(n, nv, bold_series, seed_index):
    _, length, columns = bold_series.shape
    count = seed_index.shape[0]
    block = columns // n
    steps = n // 4 * pieces
    width = block // pieces
    padded = -(-length // 128) * 128
    chunk = 1024
    i16 = jnp.int16
    dma = pltpu.SemaphoreType.DMA
    result = pl.pallas_call(
        functools.partial(kernel, n, nv, chunk),
        out_shape=pltpu.VMEM((block, count), jnp.float32),
        in_specs=[pl.BlockSpec(memory_space=pltpu.HBM), pl.BlockSpec(memory_space=pltpu.HBM)],
        out_specs=pl.BlockSpec(memory_space=pltpu.VMEM),
        scratch_shapes=[
            pltpu.VMEM((1, count), jnp.int32),
            pltpu.VMEM((count, block), jnp.float32),
            pltpu.VMEM((columns // 128, length, 128), jnp.float32),
            pltpu.VMEM((length, columns), jnp.bfloat16),
            pltpu.VMEM((padded, count), jnp.float32),
            pltpu.VMEM((length, count), jnp.bfloat16),
            pltpu.VMEM((nv - 1, length, count), jnp.bfloat16),
            pltpu.VMEM((count, padded), jnp.bfloat16),
            pltpu.VMEM((2 * steps, count, width), i16),
            pltpu.VMEM((2 * steps, count, width), i16),
            pltpu.VMEM((steps, count, width), i16),
            pltpu.VMEM((steps, count, width), i16),
            pltpu.VMEM((steps - pieces, count, width), i16),
            pltpu.VMEM((steps - pieces, count, width), i16),
            dma((columns // 128,)), dma,
            dma((nv - 1,)), dma((nv - 1,)),
            dma((2 * steps,)), dma((2 * steps,)),
            dma((steps,)), dma((steps,)),
            dma((steps - pieces,)), dma((steps - pieces,)),
        ],
        compiler_params=pltpu.CompilerParams(
            collective_id=0, has_side_effects=True, vmem_limit_bytes=60000 * 1024
        ),
    )(bold_series.reshape(length, columns // 128, 128), seed_index[None, :])
    return result


def solution(mesh):
    n, nv = mesh.shape["subj"], mesh.shape["vox"]
    in_specs = (P("subj", None, "vox"), P())
    out_specs = P(("vox", "subj"), None)
    return jax.shard_map(
        functools.partial(body, n, nv), mesh=mesh, in_specs=in_specs, out_specs=out_specs,
        check_vma=False,
    )
```

```python
import functools
import math

import jax
import jax.numpy as jnp
from jax import lax
from jax.experimental import pallas as pl
from jax.experimental.pallas import tpu as pltpu
from jax.sharding import PartitionSpec as P

clip_limit = 0.99
epsilon = 1e-05
MESH = pl.DeviceIdType.MESH
z_limit = 0.5 * math.log((1.0 + clip_limit) / (1.0 - clip_limit))
code_top = 32700.0
pieces = 2
ahead = 2
layers = 4
side_rows = 48


def encode(value, terms):
    scale = code_top / math.sqrt(terms * z_limit)
    root = value * lax.rsqrt(jnp.maximum(jnp.abs(value), 1e-30))
    return jnp.round(root * scale).astype(jnp.int32).astype(jnp.int16)


def decode(code, terms):
    scale = math.sqrt(terms * z_limit) / code_top
    root = code.astype(jnp.int32).astype(jnp.float32) * scale
    return root * jnp.abs(root)


def kernel(n, nv, chunk, side, bold, index, result, seeds, out, raw, norm, acc, pan_out, pan_in, pan_t,
           s1_out, s1_in, s2_out, s2_in, s3_out, s3_in, za_out, za_in, zb_out, zb_in,
           ta_out, ta_in, tb_out, tb_in,
           load_sem, seed_sem, p_send, p_recv, a_send, a_recv, b_send, b_recv, c_send, c_recv,
           za_send, za_recv, zb_send, zb_recv, ta_send, ta_recv, tb_send, tb_recv):
    length, columns = norm.shape
    block = columns // n
    hi_count = n // 4
    steps = hi_count * pieces
    width = block // pieces
    main = pl.ds(side, seeds.shape[1] - side)
    side_turn = 7
    offsets = sorted(range(hi_count), key=lambda d: -min(d, hi_count - d))
    s = lax.axis_index("subj")
    v = lax.axis_index("vox")
    odd = lax.rem(v, 2)
    w1, w2 = 1 + odd, 2 - odd
    f, g = lax.rem(s // w1, 2), lax.rem(s // w2, 2)
    hi, lo = s // 4, lax.rem(s, 4)
    mate1 = s + w1 * (1 - 2 * f)
    mate2 = s + w2 * (1 - 2 * g)

    loads, lines = columns // chunk, chunk // 128

    def load(i, j):
        line = i * lines + j
        return pltpu.make_async_copy(bold.at[:, line, :], raw.at[line], load_sem.at[line])

    fetch = pltpu.make_async_copy(index, seeds, seed_sem)
    fetch.start()
    for i in range(loads):
        for j in range(lines):
            load(i, j).start()

    barrier = pltpu.get_barrier_semaphore()
    pl.semaphore_signal(barrier, inc=1, device_id={"subj": mate1}, device_id_type=MESH)
    pl.semaphore_signal(barrier, inc=1, device_id={"subj": mate2}, device_id_type=MESH)
    for j in range(1, hi_count):
        peer = lax.rem(hi + j, hi_count) * 4 + lo
        pl.semaphore_signal(barrier, inc=1, device_id={"subj": peer}, device_id_type=MESH)
    for j in range(1, nv):
        pl.semaphore_signal(
            barrier, inc=1, device_id={"vox": lax.rem(v + j, nv)}, device_id_type=MESH
        )

    acc[...] = jnp.zeros_like(acc)

    def arrive(i):
        for j in range(lines):
            load(i, j).wait()

    def normalize(i):
        for j in range(lines):
            line = i * lines + j
            cols = pl.ds(pl.multiple_of(line * 128, 128), 128)
            x = raw[line]
            x = x - jnp.sum(x, axis=0, keepdims=True) * (1.0 / length)
            spread = jnp.sum(x * x, axis=0, keepdims=True) * (1.0 / length)
            norm[:, cols] = (x * lax.rsqrt(spread + epsilon)).astype(jnp.bfloat16)

    def pick(i):
        cols = pl.ds(pl.multiple_of(i * chunk, 128), chunk)
        rows = lax.broadcasted_iota(jnp.int16, (chunk, seeds.shape[1]), 0)
        place = jnp.clip(seeds[...] - (v * columns + i * chunk), -1, chunk).astype(jnp.int16)
        hit = jnp.where(rows == place, jnp.bfloat16(1.0), jnp.bfloat16(0.0))
        acc[pl.ds(0, length), :] += jnp.dot(
            norm[:, cols], hit, preferred_element_type=jnp.float32,
        )

    fetch.wait()
    arrive(0)
    normalize(0)

    @pl.loop(1, loads)
    def _(i):
        arrive(i)
        pick(i - 1)
        normalize(i)

    pick(loads - 1)

    pl.semaphore_wait(barrier, 2 + (hi_count - 1) + (nv - 1))
    pan_out[...] = acc[pl.ds(0, length), :].astype(jnp.bfloat16)

    def panel_copy(j):
        return pltpu.make_async_remote_copy(
            src_ref=pan_out, dst_ref=pan_in.at[j - 1],
            send_sem=p_send.at[j - 1], recv_sem=p_recv.at[j - 1],
            device_id={"vox": lax.rem(v + j, nv)}, device_id_type=MESH,
        )

    for j in range(1, nv):
        panel_copy(j).start()
    for j in range(1, nv):
        panel_copy(j).wait_recv()
        acc[pl.ds(0, length), :] += pan_in[j - 1].astype(jnp.float32)
    pan_t[...] = acc[...].T.astype(jnp.bfloat16)

    def target_of(step):
        turn = step // pieces
        offset = 0
        for place, d in enumerate(offsets):
            offset = offset + jnp.where(turn == place, d, 0)
        return lax.rem(hi + offset, hi_count)

    def correlate(rows, cols):
        cross = jnp.dot(
            pan_t[rows, pl.ds(0, length)], norm[:, cols], preferred_element_type=jnp.float32
        )
        c = jnp.clip(cross * (1.0 / length), -clip_limit, clip_limit)
        return 0.5 * (jnp.log(1.0 + c) - jnp.log(1.0 - c))

    def fisher(step, gg, ff):
        start = (target_of(step) * 4 + gg * w2 + ff * w1) * block
        start = start + lax.rem(step, pieces) * width
        return correlate(main, pl.ds(pl.multiple_of(start, 128), width))

    def copy1(k):
        return pltpu.make_async_remote_copy(
            src_ref=s1_out.at[k], dst_ref=s1_in.at[k], send_sem=a_send.at[k],
            recv_sem=a_recv.at[k], device_id={"subj": mate1}, device_id_type=MESH,
        )

    def copy2(k):
        return pltpu.make_async_remote_copy(
            src_ref=s2_out.at[k], dst_ref=s2_in.at[k], send_sem=b_send.at[k],
            recv_sem=b_recv.at[k], device_id={"subj": mate2}, device_id_type=MESH,
        )

    def copy3(k):
        target = target_of(k) * 4 + lo
        return pltpu.make_async_remote_copy(
            src_ref=s3_out.at[k], dst_ref=s3_in.at[k], send_sem=c_send.at[k],
            recv_sem=c_recv.at[k], device_id={"subj": target}, device_id_type=MESH,
        )

    pair = hi // 2
    inner = lax.rem((hi + 1) // 2, 2)
    keep = inner * (1 - pair) + (1 - inner) * pair
    beside = hi + 1 - 2 * lax.rem(hi, 2)
    beyond = hi + 2 - 4 * pair

    def side_fisher(which, e):
        first = 1 - jnp.minimum(e // 4, 1)
        layer = 2 * which + first * (1 - pair) + (1 - first) * pair
        start = (layer * 4 + lax.rem(e, 4)) * block
        return correlate(pl.ds(0, side), pl.ds(pl.multiple_of(start, 128), block))

    def copy_za(e):
        return pltpu.make_async_remote_copy(
            src_ref=za_out.at[e], dst_ref=za_in.at[e], send_sem=za_send.at[e],
            recv_sem=za_recv.at[e], device_id={"subj": beside * 4 + lo}, device_id_type=MESH,
        )

    def copy_zb(e):
        first = 1 - jnp.minimum(e // 4, 1)
        target = first * (inner * beyond + (1 - inner) * beside) + (1 - first) * (3 - hi)
        slot = lax.rem(e, 4) + 4 * inner
        return pltpu.make_async_remote_copy(
            src_ref=zb_out.at[e], dst_ref=zb_in.at[slot], send_sem=zb_send.at[e],
            recv_sem=zb_recv.at[slot], device_id={"subj": target * 4 + lo}, device_id_type=MESH,
        )

    def arrived_zb(slot):
        pltpu.make_async_remote_copy(
            src_ref=zb_out.at[slot], dst_ref=zb_in.at[slot], send_sem=zb_send.at[slot],
            recv_sem=zb_recv.at[slot], device_id={"subj": mate1}, device_id_type=MESH,
        ).wait_recv()

    def copy_ta(k):
        return pltpu.make_async_remote_copy(
            src_ref=ta_out.at[k], dst_ref=ta_in.at[k], send_sem=ta_send.at[k],
            recv_sem=ta_recv.at[k], device_id={"subj": mate1}, device_id_type=MESH,
        )

    def copy_tb():
        return pltpu.make_async_remote_copy(
            src_ref=tb_out, dst_ref=tb_in, send_sem=tb_send,
            recv_sem=tb_recv, device_id={"subj": mate2}, device_id_type=MESH,
        )

    def layer_sum(gg, ff):
        q = gg * w2 + ff * w1
        return decode(zb_in[q], 2) + decode(zb_in[q + 4], 2)

    @pl.loop(0, steps + ahead + 1)
    def _(turn):
        @pl.when(turn < steps)
        def _():
            s1_out[2 * turn] = encode(fisher(turn, 1 - g, 1 - f), 1)
            copy1(2 * turn).start()
            s1_out[2 * turn + 1] = encode(fisher(turn, g, 1 - f), 1)
            copy1(2 * turn + 1).start()

        if side:
            @pl.when(turn < 4)
            def _():
                @pl.loop(2 * turn, 2 * turn + 2)
                def _(e):
                    za_out[e] = encode(side_fisher(1 - keep, e), 1)
                    copy_za(e).start()

        @pl.when((turn >= ahead) & (turn < steps + ahead))
        def _():
            k = turn - ahead
            mine = fisher(k, 1 - g, f)
            copy1(2 * k).wait_recv()
            s2_out[k] = encode(mine + decode(s1_in[2 * k], 1), 2)
            copy2(k).start()

        if side:
            @pl.when((turn >= 2) & (turn < 6))
            def _():
                @pl.loop(2 * turn - 4, 2 * turn - 2)
                def _(e):
                    mine = side_fisher(keep, e)
                    copy_za(e).wait_recv()
                    code = encode(mine + decode(za_in[e], 1), 2)

                    @pl.when((inner == 0) & (e >= 4))
                    def _():
                        zb_in[e - 4] = code

                    @pl.when((inner == 1) | (e < 4))
                    def _():
                        zb_out[e] = code
                        copy_zb(e).start()

            @pl.when(turn == side_turn)
            def _():
                for q in range(4):
                    @pl.when(inner == 1)
                    def _():
                        arrived_zb(q)

                    arrived_zb(q + 4)
                ta_out[0] = encode(layer_sum(1 - g, 1 - f), 4)
                copy_ta(0).start()
                ta_out[1] = encode(layer_sum(g, 1 - f), 4)
                copy_ta(1).start()

            @pl.when(turn == side_turn + 1)
            def _():
                copy_ta(0).wait_recv()
                tb_out[...] = encode(layer_sum(1 - g, f) + decode(ta_in[0], 4), 8)
                copy_tb().start()

            @pl.when(turn == side_turn + 2)
            def _():
                copy_ta(1).wait_recv()
                copy_tb().wait_recv()
                total = layer_sum(g, f) + decode(ta_in[1], 4) + decode(tb_in[...], 8)
                out[pl.ds(0, side), :] = total * (1.0 / n)

        @pl.when(turn >= ahead + 1)
        def _():
            k = turn - ahead - 1
            mine = fisher(k, g, f)
            copy1(2 * k + 1).wait_recv()
            mine = mine + decode(s1_in[2 * k + 1], 1)
            copy2(k).wait_recv()
            mine = mine + decode(s2_in[k], 2)

            @pl.when(k < steps - pieces)
            def _():
                s3_out[k] = encode(mine, 4)
                copy3(k).start()

            @pl.when(k >= steps - pieces)
            def _():
                cols = pl.ds(pl.multiple_of((k - steps + pieces) * width, 128), width)
                out[main, cols] = mine

    for p in range(pieces):
        cols = pl.ds(p * width, width)
        for k in range(p, steps - pieces, pieces):
            copy3(k).wait_recv()
        total = out[main, cols]
        for k in range(p, steps - pieces, pieces):
            total = total + decode(s3_in[k], 4)
        out[main, cols] = total * (1.0 / n)
        result[cols, :] = out[:, cols].T

    if side:
        @pl.loop(0, 8)
        def _(e):
            copy_za(e).wait_send()

            @pl.when((inner == 1) | (e < 4))
            def _():
                copy_zb(e).wait_send()

        copy_ta(0).wait_send()
        copy_ta(1).wait_send()
        copy_tb().wait_send()

    for j in range(1, nv):
        panel_copy(j).wait_send()

    @pl.loop(0, 2 * steps)
    def _(k):
        copy1(k).wait_send()

    @pl.loop(0, steps)
    def _(k):
        copy2(k).wait_send()

    @pl.loop(0, steps - pieces)
    def _(k):
        copy3(k).wait_send()


def body(n, nv, bold_series, seed_index):
    _, length, columns = bold_series.shape
    count = seed_index.shape[0]
    block = columns // n
    steps = n // 4 * pieces
    width = block // pieces
    padded = -(-length // 128) * 128
    chunk = 1024
    side = side_rows if n // 4 == layers else 0
    rest, part = count - side, max(side, 16)
    i16 = jnp.int16
    dma = pltpu.SemaphoreType.DMA
    result = pl.pallas_call(
        functools.partial(kernel, n, nv, chunk, side),
        out_shape=pltpu.VMEM((block, count), jnp.float32),
        in_specs=[pl.BlockSpec(memory_space=pltpu.HBM), pl.BlockSpec(memory_space=pltpu.HBM)],
        out_specs=pl.BlockSpec(memory_space=pltpu.VMEM),
        scratch_shapes=[
            pltpu.VMEM((1, count), jnp.int32),
            pltpu.VMEM((count, block), jnp.float32),
            pltpu.VMEM((columns // 128, length, 128), jnp.float32),
            pltpu.VMEM((length, columns), jnp.bfloat16),
            pltpu.VMEM((padded, count), jnp.float32),
            pltpu.VMEM((length, count), jnp.bfloat16),
            pltpu.VMEM((nv - 1, length, count), jnp.bfloat16),
            pltpu.VMEM((count, padded), jnp.bfloat16),
            pltpu.VMEM((2 * steps, rest, width), i16),
            pltpu.VMEM((2 * steps, rest, width), i16),
            pltpu.VMEM((steps, rest, width), i16),
            pltpu.VMEM((steps, rest, width), i16),
            pltpu.VMEM((steps - pieces, rest, width), i16),
            pltpu.VMEM((steps - pieces, rest, width), i16),
            pltpu.VMEM((8, part, block), i16),
            pltpu.VMEM((8, part, block), i16),
            pltpu.VMEM((8, part, block), i16),
            pltpu.VMEM((8, part, block), i16),
            pltpu.VMEM((2, part, block), i16),
            pltpu.VMEM((2, part, block), i16),
            pltpu.VMEM((part, block), i16),
            pltpu.VMEM((part, block), i16),
            dma((columns // 128,)), dma,
            dma((nv - 1,)), dma((nv - 1,)),
            dma((2 * steps,)), dma((2 * steps,)),
            dma((steps,)), dma((steps,)),
            dma((steps - pieces,)), dma((steps - pieces,)),
            dma((8,)), dma((8,)),
            dma((8,)), dma((8,)),
            dma((2,)), dma((2,)),
            dma, dma,
        ],
        compiler_params=pltpu.CompilerParams(
            collective_id=0, has_side_effects=True, vmem_limit_bytes=60000 * 1024
        ),
    )(bold_series.reshape(length, columns // 128, 128), seed_index[None, :])
    return result


def solution(mesh):
    n, nv = mesh.shape["subj"], mesh.shape["vox"]
    in_specs = (P("subj", None, "vox"), P())
    out_specs = P(("vox", "subj"), None)
    return jax.shard_map(
        functools.partial(body, n, nv), mesh=mesh, in_specs=in_specs, out_specs=out_specs,
        check_vma=False,
    )
```

```python
import functools
import math

import jax
import jax.numpy as jnp
from jax import lax
from jax.experimental import pallas as pl
from jax.experimental.pallas import tpu as pltpu
from jax.sharding import PartitionSpec as P

clip_limit = 0.99
epsilon = 1e-05
MESH = pl.DeviceIdType.MESH
z_limit = 0.5 * math.log((1.0 + clip_limit) / (1.0 - clip_limit))
code_top = 32700.0
pieces = 2
ahead = 2
last = 4
layers = 4
deep = 3
side_rows = 48


def encode(value, terms):
    scale = code_top / math.sqrt(terms * z_limit)
    root = value * lax.rsqrt(jnp.maximum(jnp.abs(value), 1e-30))
    return jnp.round(root * scale).astype(jnp.int32).astype(jnp.int16)


def decode(code, terms):
    scale = math.sqrt(terms * z_limit) / code_top
    root = code.astype(jnp.int32).astype(jnp.float32) * scale
    return root * jnp.abs(root)


def kernel(n, nv, chunk, side, bold, index, result, seeds, out, raw, norm, acc, pan_out, pan_in, pan_t,
           s1_out, s1_in, s2_out, s2_in, s3_out, s3_in, za_out, za_in, zb_out, zb_in,
           ta_out, ta_in, tb_out, tb_in, hold, x_out, x_in,
           load_sem, seed_sem, p_send, p_recv, a_send, a_recv, b_send, b_recv, c_send, c_recv,
           za_send, za_recv, zb_send, zb_recv, ta_send, ta_recv, tb_send, tb_recv, x_send, x_recv):
    length, columns = norm.shape
    block = columns // n
    hi_count = n // 4
    steps = hi_count * pieces
    width = block // pieces
    main = pl.ds(side, seeds.shape[1] - side)
    far, cross = 2 * pieces, 2
    side_start, side_turn, side_next, side_end = 2, 7, 9, 11
    offsets = sorted(range(hi_count), key=lambda d: -min(d, hi_count - d))
    s = lax.axis_index("subj")
    v = lax.axis_index("vox")
    odd = lax.rem(v, 2)
    w1, w2 = 1 + odd, 2 - odd
    f, g = lax.rem(s // w1, 2), lax.rem(s // w2, 2)
    hi, lo = s // 4, lax.rem(s, 4)
    mate1 = s + w1 * (1 - 2 * f)
    mate2 = s + w2 * (1 - 2 * g)

    loads, lines = columns // chunk, chunk // 128

    def load(i, j):
        line = i * lines + j
        return pltpu.make_async_copy(bold.at[:, line, :], raw.at[line], load_sem.at[line])

    fetch = pltpu.make_async_copy(index, seeds, seed_sem)
    fetch.start()
    def begin(i):
        for j in range(lines):
            load(i, j).start()

    for i in range(deep):
        begin(i)

    barrier = pltpu.get_barrier_semaphore()
    pl.semaphore_signal(barrier, inc=1, device_id={"subj": mate1}, device_id_type=MESH)
    pl.semaphore_signal(barrier, inc=1, device_id={"subj": mate2}, device_id_type=MESH)
    for j in range(1, hi_count):
        peer = lax.rem(hi + j, hi_count) * 4 + lo
        pl.semaphore_signal(barrier, inc=1, device_id={"subj": peer}, device_id_type=MESH)
    for j in range(1, nv):
        pl.semaphore_signal(
            barrier, inc=1, device_id={"vox": lax.rem(v + j, nv)}, device_id_type=MESH
        )

    acc[...] = jnp.zeros_like(acc)

    def arrive(i):
        for j in range(lines):
            load(i, j).wait()

    def normalize(i):
        for j in range(lines):
            line = i * lines + j
            cols = pl.ds(pl.multiple_of(line * 128, 128), 128)
            x = raw[line]
            x = x - jnp.sum(x, axis=0, keepdims=True) * (1.0 / length)
            spread = jnp.sum(x * x, axis=0, keepdims=True) * (1.0 / length)
            norm[:, cols] = (x * lax.rsqrt(spread + epsilon)).astype(jnp.bfloat16)

    def pick(i):
        cols = pl.ds(pl.multiple_of(i * chunk, 128), chunk)
        rows = lax.broadcasted_iota(jnp.int16, (chunk, seeds.shape[1]), 0)
        place = jnp.clip(seeds[...] - (v * columns + i * chunk), -1, chunk).astype(jnp.int16)
        hit = jnp.where(rows == place, jnp.bfloat16(1.0), jnp.bfloat16(0.0))
        acc[pl.ds(0, length), :] += jnp.dot(
            norm[:, cols], hit, preferred_element_type=jnp.float32,
        )

    fetch.wait()
    arrive(0)
    begin(min(deep, loads - 1)) if deep < loads else None
    normalize(0)

    @pl.loop(1, loads)
    def _(i):
        arrive(i)

        @pl.when(i + deep < loads)
        def _():
            begin(i + deep)

        pick(i - 1)
        normalize(i)

    pick(loads - 1)

    pl.semaphore_wait(barrier, 2 + (hi_count - 1) + (nv - 1))
    pan_out[...] = acc[pl.ds(0, length), :].astype(jnp.bfloat16)

    def panel_copy(j):
        return pltpu.make_async_remote_copy(
            src_ref=pan_out, dst_ref=pan_in.at[j - 1],
            send_sem=p_send.at[j - 1], recv_sem=p_recv.at[j - 1],
            device_id={"vox": lax.rem(v + j, nv)}, device_id_type=MESH,
        )

    for j in range(1, nv):
        panel_copy(j).start()
    for j in range(1, nv):
        panel_copy(j).wait_recv()
        acc[pl.ds(0, length), :] += pan_in[j - 1].astype(jnp.float32)
    pan_t[...] = acc[...].T.astype(jnp.bfloat16)

    pair = hi // 2
    inner = lax.rem((hi + 1) // 2, 2)
    beside = hi + 1 - 2 * lax.rem(hi, 2)

    def target_of(step):
        turn = step // pieces
        order = [3 - 3 * pair, 2 - pair, beside, hi] if side else [
            lax.rem(hi + d, hi_count) for d in offsets
        ]
        layer = 0
        for place, h in enumerate(order):
            layer = layer + jnp.where(turn == place, h, 0)
        return layer

    def correlate(rows, cols):
        cross = jnp.dot(
            pan_t[rows, pl.ds(0, length)], norm[:, cols], preferred_element_type=jnp.float32
        )
        c = jnp.clip(cross * (1.0 / length), -clip_limit, clip_limit)
        return 0.5 * (jnp.log(1.0 + c) - jnp.log(1.0 - c))

    def fisher(step, gg, ff):
        start = (target_of(step) * 4 + gg * w2 + ff * w1) * block
        start = start + lax.rem(step, pieces) * width
        return correlate(main, pl.ds(pl.multiple_of(start, 128), width))

    def copy1(k):
        return pltpu.make_async_remote_copy(
            src_ref=s1_out.at[k], dst_ref=s1_in.at[k], send_sem=a_send.at[k],
            recv_sem=a_recv.at[k], device_id={"subj": mate1}, device_id_type=MESH,
        )

    def copy2(k):
        return pltpu.make_async_remote_copy(
            src_ref=s2_out.at[k], dst_ref=s2_in.at[k], send_sem=b_send.at[k],
            recv_sem=b_recv.at[k], device_id={"subj": mate2}, device_id_type=MESH,
        )

    def copy3(k):
        target = target_of(k) * 4 + lo
        return pltpu.make_async_remote_copy(
            src_ref=s3_out.at[k], dst_ref=s3_in.at[k], send_sem=c_send.at[k],
            recv_sem=c_recv.at[k], device_id={"subj": target}, device_id_type=MESH,
        )

    def copy_z(k):
        return pltpu.make_async_remote_copy(
            src_ref=s3_out.at[k], dst_ref=s3_in.at[k], send_sem=c_send.at[k],
            recv_sem=c_recv.at[k], device_id={"subj": beside * 4 + lo}, device_id_type=MESH,
        )

    def copy_x(k):
        slot = lax.rem(k, pieces)
        return pltpu.make_async_remote_copy(
            src_ref=x_out.at[k], dst_ref=x_in.at[slot], send_sem=x_send.at[k],
            recv_sem=x_recv.at[slot], device_id={"subj": target_of(k) * 4 + lo},
            device_id_type=MESH,
        )

    def far_layer(e):
        return 3 - 3 * pair + (e // 4) * (2 * pair - 1)

    def side_fisher(layer, q):
        start = (layer * 4 + q) * block
        return correlate(pl.ds(0, side), pl.ds(pl.multiple_of(start, 128), block))

    def copy_za(e):
        return pltpu.make_async_remote_copy(
            src_ref=za_out.at[e], dst_ref=za_in.at[e], send_sem=za_send.at[e],
            recv_sem=za_recv.at[e], device_id={"subj": beside * 4 + lo}, device_id_type=MESH,
        )

    def copy_zb(e):
        slot = lax.rem(e, 4)
        return pltpu.make_async_remote_copy(
            src_ref=zb_out.at[e], dst_ref=zb_in.at[slot], send_sem=zb_send.at[e],
            recv_sem=zb_recv.at[slot], device_id={"subj": far_layer(e) * 4 + lo},
            device_id_type=MESH,
        )

    def copy_ta(k):
        return pltpu.make_async_remote_copy(
            src_ref=ta_out.at[k], dst_ref=ta_in.at[k], send_sem=ta_send.at[k],
            recv_sem=ta_recv.at[k], device_id={"subj": mate2}, device_id_type=MESH,
        )

    def copy_tb():
        return pltpu.make_async_remote_copy(
            src_ref=tb_out, dst_ref=tb_in, send_sem=tb_send,
            recv_sem=tb_recv, device_id={"subj": mate1}, device_id_type=MESH,
        )

    def layer_sum(gg, ff):
        q = gg * w2 + ff * w1
        return side_fisher(hi, q) + decode(za_in[q + 8], 1) + decode(zb_in[q], 2)

    @pl.loop(0, steps + last)
    def _(turn):
        @pl.when(turn < steps)
        def _():
            s1_out[2 * turn] = encode(fisher(turn, 1 - g, 1 - f), 1)
            copy1(2 * turn).start()
            s1_out[2 * turn + 1] = encode(fisher(turn, g, 1 - f), 1)
            copy1(2 * turn + 1).start()

        if side:
            @pl.when((turn < 2) & (inner == 0))
            def _():
                @pl.loop(4 * turn, 4 * turn + 4)
                def _(e):
                    za_out[e] = encode(side_fisher(far_layer(e), lax.rem(e, 4)), 1)
                    copy_za(e).start()

            @pl.when(turn == 2 - 2 * inner)
            def _():
                @pl.loop(0, 4)
                def _(q):
                    za_out[q + 8] = encode(side_fisher(beside, q), 1)
                    copy_za(q + 8).start()

        @pl.when((turn >= ahead) & (turn < steps + ahead))
        def _():
            k = turn - ahead
            mine = fisher(k, 1 - g, f)
            copy1(2 * k).wait_recv()
            s2_out[k] = encode(mine + decode(s1_in[2 * k], 1), 2)
            copy2(k).start()

        if side:
            @pl.when((turn >= side_start) & (turn < side_start + 4) & (inner == 1))
            def _():
                @pl.loop(2 * (turn - side_start), 2 * (turn - side_start) + 2)
                def _(e):
                    mine = side_fisher(far_layer(e), lax.rem(e, 4))
                    copy_za(e).wait_recv()
                    zb_out[e] = encode(mine + decode(za_in[e], 1), 2)
                    copy_zb(e).start()

            @pl.when(turn == side_turn)
            def _():
                for q in range(4):
                    copy_za(q + 8).wait_recv()
                    copy_zb(q).wait_recv()
                ta_out[0] = encode(layer_sum(1 - g, 1 - f), 4)
                copy_ta(0).start()
                ta_out[1] = encode(layer_sum(1 - g, f), 4)
                copy_ta(1).start()

            @pl.when(turn == side_next)
            def _():
                copy_ta(0).wait_recv()
                tb_out[...] = encode(layer_sum(g, 1 - f) + decode(ta_in[0], 4), 8)
                copy_tb().start()

            @pl.when(turn == side_end)
            def _():
                copy_ta(1).wait_recv()
                copy_tb().wait_recv()
                total = layer_sum(g, f) + decode(ta_in[1], 4) + decode(tb_in[...], 8)
                out[pl.ds(0, side), :] = total * (1.0 / n)

                @pl.loop(0, 8)
                def _(e):
                    @pl.when(inner == 0)
                    def _():
                        copy_za(e).wait_send()

                    @pl.when(inner == 1)
                    def _():
                        copy_zb(e).wait_send()

                for q in range(4):
                    copy_za(q + 8).wait_send()

                copy_ta(0).wait_send()
                copy_ta(1).wait_send()
                copy_tb().wait_send()

        @pl.when(turn >= last)
        def _():
            k = turn - last
            mine = fisher(k, g, f)
            copy1(2 * k + 1).wait_recv()
            mine = mine + decode(s1_in[2 * k + 1], 1)
            copy2(k).wait_recv()
            mine = mine + decode(s2_in[k], 2)
            copy1(2 * k).wait_send()
            copy1(2 * k + 1).wait_send()
            copy2(k).wait_send()

            if side:
                @pl.when((k < steps - pieces) & ((inner == 0) | (k >= far)))
                def _():
                    s3_out[k] = encode(mine, 4)
                    copy_z(k).start()

                @pl.when((k < far) & (inner == 1))
                def _():
                    hold[k] = mine
            else:
                @pl.when(k < steps - pieces)
                def _():
                    s3_out[k] = encode(mine, 4)
                    copy3(k).start()

            @pl.when(k >= steps - pieces)
            def _():
                cols = pl.ds(pl.multiple_of((k - steps + pieces) * width, 128), width)
                out[main, cols] = mine

        if side:
            @pl.when((turn >= last + cross) & (turn < last + cross + far) & (inner == 1))
            def _():
                k = turn - last - cross
                copy_z(k).wait_recv()
                x_out[k] = encode(hold[k] + decode(s3_in[k], 4), 8)
                copy_x(k).start()

    for p in range(pieces):
        cols = pl.ds(p * width, width)
        total = out[main, cols]
        if side:
            copy_z(far + p).wait_recv()
            copy_x(p).wait_recv()
            total = total + decode(s3_in[far + p], 4) + decode(x_in[p], 8)
        else:
            for k in range(p, steps - pieces, pieces):
                copy3(k).wait_recv()
                total = total + decode(s3_in[k], 4)
        out[main, cols] = total * (1.0 / n)
        result[cols, :] = out[:, cols].T

    for j in range(1, nv):
        panel_copy(j).wait_send()

    if side:
        @pl.loop(0, far)
        def _(k):
            @pl.when(inner == 0)
            def _():
                copy_z(k).wait_send()

            @pl.when(inner == 1)
            def _():
                copy_x(k).wait_send()

        for p in range(pieces):
            copy_z(far + p).wait_send()
    else:
        @pl.loop(0, steps - pieces)
        def _(k):
            copy3(k).wait_send()


def body(n, nv, bold_series, seed_index):
    _, length, columns = bold_series.shape
    count = seed_index.shape[0]
    block = columns // n
    steps = n // 4 * pieces
    width = block // pieces
    padded = -(-length // 128) * 128
    chunk = 1024
    side = side_rows if n // 4 == layers else 0
    rest, part = count - side, max(side, 16)
    i16 = jnp.int16
    dma = pltpu.SemaphoreType.DMA
    result = pl.pallas_call(
        functools.partial(kernel, n, nv, chunk, side),
        out_shape=pltpu.VMEM((block, count), jnp.float32),
        in_specs=[pl.BlockSpec(memory_space=pltpu.HBM), pl.BlockSpec(memory_space=pltpu.HBM)],
        out_specs=pl.BlockSpec(memory_space=pltpu.VMEM),
        scratch_shapes=[
            pltpu.VMEM((1, count), jnp.int32),
            pltpu.VMEM((count, block), jnp.float32),
            pltpu.VMEM((columns // 128, length, 128), jnp.float32),
            pltpu.VMEM((length, columns), jnp.bfloat16),
            pltpu.VMEM((padded, count), jnp.float32),
            pltpu.VMEM((length, count), jnp.bfloat16),
            pltpu.VMEM((nv - 1, length, count), jnp.bfloat16),
            pltpu.VMEM((count, padded), jnp.bfloat16),
            pltpu.VMEM((2 * steps, rest, width), i16),
            pltpu.VMEM((2 * steps, rest, width), i16),
            pltpu.VMEM((steps, rest, width), i16),
            pltpu.VMEM((steps, rest, width), i16),
            pltpu.VMEM((steps - pieces, rest, width), i16),
            pltpu.VMEM((steps - pieces, rest, width), i16),
            pltpu.VMEM((12, part, block), i16),
            pltpu.VMEM((12, part, block), i16),
            pltpu.VMEM((8, part, block), i16),
            pltpu.VMEM((4, part, block), i16),
            pltpu.VMEM((2, part, block), i16),
            pltpu.VMEM((2, part, block), i16),
            pltpu.VMEM((part, block), i16),
            pltpu.VMEM((part, block), i16),
            pltpu.VMEM((2 * pieces, rest, width), jnp.float32),
            pltpu.VMEM((2 * pieces, rest, width), i16),
            pltpu.VMEM((pieces, rest, width), i16),
            dma((columns // 128,)), dma,
            dma((nv - 1,)), dma((nv - 1,)),
            dma((2 * steps,)), dma((2 * steps,)),
            dma((steps,)), dma((steps,)),
            dma((steps - pieces,)), dma((steps - pieces,)),
            dma((12,)), dma((12,)),
            dma((8,)), dma((4,)),
            dma((2,)), dma((2,)),
            dma, dma,
            dma((2 * pieces,)), dma((pieces,)),
        ],
        compiler_params=pltpu.CompilerParams(
            collective_id=0, has_side_effects=True, vmem_limit_bytes=60000 * 1024
        ),
    )(bold_series.reshape(length, columns // 128, 128), seed_index[None, :])
    return result


def solution(mesh):
    n, nv = mesh.shape["subj"], mesh.shape["vox"]
    in_specs = (P("subj", None, "vox"), P())
    out_specs = P(("vox", "subj"), None)
    return jax.shard_map(
        functools.partial(body, n, nv), mesh=mesh, in_specs=in_specs, out_specs=out_specs,
        check_vma=False,
    )
```

```python
import functools
import math

import jax
import jax.numpy as jnp
from jax import lax
from jax.experimental import pallas as pl
from jax.experimental.pallas import tpu as pltpu
from jax.sharding import PartitionSpec as P

clip_limit = 0.99
epsilon = 1e-05
MESH = pl.DeviceIdType.MESH
z_limit = 0.5 * math.log((1.0 + clip_limit) / (1.0 - clip_limit))
code_top = 32700.0
pieces = 2
ahead = 3
last = 5
late = 1
layers = 4
deep = 3
side_rows = 48


def encode(value, terms):
    scale = code_top / math.sqrt(terms * z_limit)
    root = value * lax.rsqrt(jnp.maximum(jnp.abs(value), 1e-30))
    return jnp.round(root * scale).astype(jnp.int32).astype(jnp.int16)


def decode(code, terms):
    scale = math.sqrt(terms * z_limit) / code_top
    root = code.astype(jnp.int32).astype(jnp.float32) * scale
    return root * jnp.abs(root)


def kernel(n, nv, chunk, side, bold, index, result, seeds, out, raw, norm, acc, pan_out, pan_in, pan_t,
           s1_out, s1_in, s2_out, s2_in, s3_out, s3_in, za_out, za_in, zb_out, zb_in,
           ta_out, ta_in, tb_out, tb_in, hold, x_out, x_in,
           load_sem, seed_sem, p_send, p_recv, a_send, a_recv, b_send, b_recv, c_send, c_recv,
           za_send, za_recv, zb_send, zb_recv, ta_send, ta_recv, tb_send, tb_recv, x_send, x_recv):
    length, columns = norm.shape
    block = columns // n
    hi_count = n // 4
    steps = hi_count * pieces
    width = block // pieces
    main = pl.ds(side, seeds.shape[1] - side)
    far, cross = 2 * pieces, 2
    side_turn, side_next, side_end = 7, 9, 11
    offsets = sorted(range(hi_count), key=lambda d: -min(d, hi_count - d))
    s = lax.axis_index("subj")
    v = lax.axis_index("vox")
    odd = lax.rem(v, 2)
    w1, w2 = 1 + odd, 2 - odd
    f, g = lax.rem(s // w1, 2), lax.rem(s // w2, 2)
    hi, lo = s // 4, lax.rem(s, 4)
    mate1 = s + w1 * (1 - 2 * f)
    mate2 = s + w2 * (1 - 2 * g)

    loads, lines = columns // chunk, chunk // 128

    def load(i, j):
        line = i * lines + j
        return pltpu.make_async_copy(bold.at[:, line, :], raw.at[line], load_sem.at[lax.rem(i, deep)])

    fetch = pltpu.make_async_copy(index, seeds, seed_sem)
    fetch.start()
    def begin(i):
        for j in range(lines):
            load(i, j).start()

    for i in range(deep):
        begin(i)

    barrier = pltpu.get_barrier_semaphore()
    pl.semaphore_signal(barrier, inc=1, device_id={"subj": mate1}, device_id_type=MESH)
    pl.semaphore_signal(barrier, inc=1, device_id={"subj": mate2}, device_id_type=MESH)
    for j in range(1, hi_count):
        peer = lax.rem(hi + j, hi_count) * 4 + lo
        pl.semaphore_signal(barrier, inc=1, device_id={"subj": peer}, device_id_type=MESH)
    for j in range(1, nv):
        pl.semaphore_signal(
            barrier, inc=1, device_id={"vox": lax.rem(v + j, nv)}, device_id_type=MESH
        )

    acc[...] = jnp.zeros_like(acc)

    def arrive(i):
        whole = raw.at[pl.ds(i * lines, lines)]
        pltpu.make_async_copy(whole, whole, load_sem.at[lax.rem(i, deep)]).wait()

    def normalize(i):
        for j in range(lines):
            line = i * lines + j
            cols = pl.ds(pl.multiple_of(line * 128, 128), 128)
            x = raw[line]
            x = x - jnp.sum(x, axis=0, keepdims=True) * (1.0 / length)
            spread = jnp.sum(x * x, axis=0, keepdims=True) * (1.0 / length)
            norm[:, cols] = (x * lax.rsqrt(spread + epsilon)).astype(jnp.bfloat16)

    def pick(i):
        cols = pl.ds(pl.multiple_of(i * chunk, 128), chunk)
        rows = lax.broadcasted_iota(jnp.int16, (chunk, seeds.shape[1]), 0)
        place = jnp.clip(seeds[...] - (v * columns + i * chunk), -1, chunk).astype(jnp.int16)
        hit = jnp.where(rows == place, jnp.bfloat16(1.0), jnp.bfloat16(0.0))
        acc[pl.ds(0, length), :] += jnp.dot(
            norm[:, cols], hit, preferred_element_type=jnp.float32,
        )

    fetch.wait()
    arrive(0)
    begin(min(deep, loads - 1)) if deep < loads else None
    normalize(0)

    @pl.loop(1, loads)
    def _(i):
        arrive(i)

        @pl.when(i + deep < loads)
        def _():
            begin(i + deep)

        pick(i - 1)
        normalize(i)

    pick(loads - 1)

    pl.semaphore_wait(barrier, 2 + (hi_count - 1) + (nv - 1))
    pan_out[...] = acc[pl.ds(0, length), :].astype(jnp.bfloat16)

    def panel_copy(j):
        return pltpu.make_async_remote_copy(
            src_ref=pan_out, dst_ref=pan_in.at[j - 1],
            send_sem=p_send.at[j - 1], recv_sem=p_recv.at[j - 1],
            device_id={"vox": lax.rem(v + j, nv)}, device_id_type=MESH,
        )

    for j in range(1, nv):
        panel_copy(j).start()
    for j in range(1, nv):
        panel_copy(j).wait_recv()
        acc[pl.ds(0, length), :] += pan_in[j - 1].astype(jnp.float32)
    pan_t[...] = acc[...].T.astype(jnp.bfloat16)

    pair = hi // 2
    inner = lax.rem((hi + 1) // 2, 2)
    beside = hi + 1 - 2 * lax.rem(hi, 2)

    def target_of(step):
        turn = step // pieces
        order = [3 - 3 * pair, 2 - pair, beside, hi] if side else [
            lax.rem(hi + d, hi_count) for d in offsets
        ]
        layer = 0
        for place, h in enumerate(order):
            layer = layer + jnp.where(turn == place, h, 0)
        return layer

    def correlate(rows, cols):
        cross = jnp.dot(
            pan_t[rows, pl.ds(0, length)], norm[:, cols], preferred_element_type=jnp.float32
        )
        c = jnp.clip(cross * (1.0 / length), -clip_limit, clip_limit)
        return 0.5 * (jnp.log(1.0 + c) - jnp.log(1.0 - c))

    def fisher(step, gg, ff):
        start = (target_of(step) * 4 + gg * w2 + ff * w1) * block
        start = start + lax.rem(step, pieces) * width
        return correlate(main, pl.ds(pl.multiple_of(start, 128), width))

    def copy1(k):
        return pltpu.make_async_remote_copy(
            src_ref=s1_out.at[k], dst_ref=s1_in.at[k], send_sem=a_send,
            recv_sem=a_recv.at[k], device_id={"subj": mate1}, device_id_type=MESH,
        )

    def copy2(k):
        return pltpu.make_async_remote_copy(
            src_ref=s2_out.at[k], dst_ref=s2_in.at[k], send_sem=b_send,
            recv_sem=b_recv.at[k], device_id={"subj": mate2}, device_id_type=MESH,
        )

    def copy3(k):
        target = target_of(k) * 4 + lo
        return pltpu.make_async_remote_copy(
            src_ref=s3_out.at[k], dst_ref=s3_in.at[k], send_sem=c_send,
            recv_sem=c_recv.at[k], device_id={"subj": target}, device_id_type=MESH,
        )

    def copy_z(k):
        return pltpu.make_async_remote_copy(
            src_ref=s3_out.at[k], dst_ref=s3_in.at[k], send_sem=c_send,
            recv_sem=c_recv.at[k], device_id={"subj": beside * 4 + lo}, device_id_type=MESH,
        )

    def copy_x(k):
        slot = lax.rem(k, pieces)
        return pltpu.make_async_remote_copy(
            src_ref=x_out.at[k], dst_ref=x_in.at[slot], send_sem=x_send,
            recv_sem=x_recv.at[slot], device_id={"subj": target_of(k) * 4 + lo},
            device_id_type=MESH,
        )

    def far_layer(e):
        return 3 - 3 * pair + (e // 4) * (2 * pair - 1)

    def side_fisher(layer, q):
        start = (layer * 4 + q) * block
        return correlate(pl.ds(0, side), pl.ds(pl.multiple_of(start, 128), block))

    def arrived(ref, sem):
        pltpu.make_async_remote_copy(
            src_ref=ref, dst_ref=ref, send_sem=tb_send, recv_sem=sem,
            device_id={"subj": mate1}, device_id_type=MESH,
        ).wait_recv()

    def copy_za(e):
        return pltpu.make_async_remote_copy(
            src_ref=za_out.at[e], dst_ref=za_in.at[e], send_sem=za_send,
            recv_sem=za_recv.at[jnp.minimum(e, 8)], device_id={"subj": beside * 4 + lo}, device_id_type=MESH,
        )

    def copy_zb(e):
        slot = lax.rem(e, 4)
        return pltpu.make_async_remote_copy(
            src_ref=zb_out.at[e], dst_ref=zb_in.at[slot], send_sem=zb_send,
            recv_sem=zb_recv, device_id={"subj": far_layer(e) * 4 + lo},
            device_id_type=MESH,
        )

    def copy_ta(k):
        return pltpu.make_async_remote_copy(
            src_ref=ta_out.at[k], dst_ref=ta_in.at[k], send_sem=ta_send,
            recv_sem=ta_recv.at[k], device_id={"subj": mate2}, device_id_type=MESH,
        )

    def copy_tb():
        return pltpu.make_async_remote_copy(
            src_ref=tb_out, dst_ref=tb_in, send_sem=tb_send,
            recv_sem=tb_recv, device_id={"subj": mate1}, device_id_type=MESH,
        )

    def layer_sum(gg, ff):
        q = gg * w2 + ff * w1
        return side_fisher(hi, q) + decode(za_in[q + 8], 1) + decode(zb_in[q], 2)

    @pl.loop(0, steps + last)
    def _(turn):
        @pl.when(turn < steps)
        def _():
            s1_out[2 * turn] = encode(fisher(turn, 1 - g, 1 - f), 1)
            copy1(2 * turn).start()

        @pl.when((turn >= late) & (turn < steps + late))
        def _():
            k = turn - late
            s1_out[2 * k + 1] = encode(fisher(k, g, 1 - f), 1)
            copy1(2 * k + 1).start()

        if side:
            @pl.when(turn == side_next)
            def _():
                copy_ta(0).wait_recv()
                tb_out[...] = encode(layer_sum(g, 1 - f) + decode(ta_in[0], 4), 8)
                copy_tb().start()

        if side:
            @pl.when((turn < 2) & (inner == 0))
            def _():
                @pl.loop(4 * turn, 4 * turn + 4)
                def _(e):
                    za_out[e] = encode(side_fisher(far_layer(e), lax.rem(e, 4)), 1)
                    copy_za(e).start()

            @pl.when(turn == 2 - 2 * inner)
            def _():
                @pl.loop(0, 4)
                def _(q):
                    za_out[q + 8] = encode(side_fisher(beside, q), 1)
                    copy_za(q + 8).start()

        @pl.when((turn >= ahead) & (turn < steps + ahead))
        def _():
            k = turn - ahead
            mine = fisher(k, 1 - g, f)
            copy1(2 * k).wait_recv()
            s2_out[k] = encode(mine + decode(s1_in[2 * k], 1), 2)
            copy2(k).start()

        if side:
            @pl.when((turn >= 2) & (turn < 5) & (inner == 1))
            def _():
                @pl.loop(2 * turn - 4, 2 * turn - 2 + 2 * (turn // 4))
                def _(e):
                    mine = side_fisher(far_layer(e), lax.rem(e, 4))
                    copy_za(e).wait_recv()
                    zb_out[e] = encode(mine + decode(za_in[e], 1), 2)
                    copy_zb(e).start()

            @pl.when(turn == side_turn)
            def _():
                arrived(za_in.at[pl.ds(8, 4)], za_recv.at[8])
                arrived(zb_in, zb_recv)
                ta_out[0] = encode(layer_sum(1 - g, 1 - f), 4)
                copy_ta(0).start()
                ta_out[1] = encode(layer_sum(1 - g, f), 4)
                copy_ta(1).start()

            @pl.when(turn == side_end)
            def _():
                copy_ta(1).wait_recv()
                copy_tb().wait_recv()
                total = layer_sum(g, f) + decode(ta_in[1], 4) + decode(tb_in[...], 8)
                out[pl.ds(0, side), :] = total * (1.0 / n)

        @pl.when(turn >= last)
        def _():
            k = turn - last
            mine = fisher(k, g, f)
            copy1(2 * k + 1).wait_recv()
            mine = mine + decode(s1_in[2 * k + 1], 1)
            copy2(k).wait_recv()
            mine = mine + decode(s2_in[k], 2)

            if side:
                @pl.when((k < steps - pieces) & ((inner == 0) | (k >= far)))
                def _():
                    s3_out[k] = encode(mine, 4)
                    copy_z(k).start()

                @pl.when((k < far) & (inner == 1))
                def _():
                    hold[k] = mine
            else:
                @pl.when(k < steps - pieces)
                def _():
                    s3_out[k] = encode(mine, 4)
                    copy3(k).start()

            @pl.when(k >= steps - pieces)
            def _():
                p = k - steps + pieces
                cols = pl.ds(pl.multiple_of(p * width, 128), width)
                if side:
                    copy_z(far + p).wait_recv()
                    copy_x(p).wait_recv()
                    total = mine + decode(s3_in[far + p], 4) + decode(x_in[p], 8)
                    out[main, cols] = total * (1.0 / n)
                    result[cols, :] = out[:, cols].T
                else:
                    out[main, cols] = mine

        if side:
            @pl.when((turn >= last + cross) & (turn < last + cross + far) & (inner == 1))
            def _():
                k = turn - last - cross
                copy_z(k).wait_recv()
                x_out[k] = encode(hold[k] + decode(s3_in[k], 4), 8)
                copy_x(k).start()

    if not side:
        for p in range(pieces):
            cols = pl.ds(p * width, width)
            total = out[main, cols]
            for k in range(p, steps - pieces, pieces):
                copy3(k).wait_recv()
                total = total + decode(s3_in[k], 4)
            out[main, cols] = total * (1.0 / n)
            result[cols, :] = out[:, cols].T

    for j in range(1, nv):
        panel_copy(j).wait_send()

    def sent(ref, sem):
        pltpu.make_async_remote_copy(
            src_ref=ref, dst_ref=ref, send_sem=sem, recv_sem=p_recv.at[0],
            device_id={"subj": mate1}, device_id_type=MESH,
        ).wait_send()

    sent(s1_out, a_send)
    sent(s2_out, b_send)
    if side:
        @pl.when(inner == 0)
        def _():
            sent(za_out, za_send)
            sent(s3_out, c_send)

        @pl.when(inner == 1)
        def _():
            sent(za_out.at[pl.ds(8, 4)], za_send)
            sent(s3_out.at[pl.ds(far, pieces)], c_send)
            sent(zb_out, zb_send)
            sent(x_out, x_send)

        sent(ta_out, ta_send)
        sent(tb_out, tb_send)
    else:
        sent(s3_out, c_send)


def body(n, nv, bold_series, seed_index):
    _, length, columns = bold_series.shape
    count = seed_index.shape[0]
    block = columns // n
    steps = n // 4 * pieces
    width = block // pieces
    padded = -(-length // 128) * 128
    chunk = 1024
    side = side_rows if n // 4 == layers else 0
    rest, part = count - side, max(side, 16)
    i16 = jnp.int16
    dma = pltpu.SemaphoreType.DMA
    result = pl.pallas_call(
        functools.partial(kernel, n, nv, chunk, side),
        out_shape=pltpu.VMEM((block, count), jnp.float32),
        in_specs=[pl.BlockSpec(memory_space=pltpu.HBM), pl.BlockSpec(memory_space=pltpu.HBM)],
        out_specs=pl.BlockSpec(memory_space=pltpu.VMEM),
        scratch_shapes=[
            pltpu.VMEM((1, count), jnp.int32),
            pltpu.VMEM((count, block), jnp.float32),
            pltpu.VMEM((columns // 128, length, 128), jnp.float32),
            pltpu.VMEM((length, columns), jnp.bfloat16),
            pltpu.VMEM((padded, count), jnp.float32),
            pltpu.VMEM((length, count), jnp.bfloat16),
            pltpu.VMEM((nv - 1, length, count), jnp.bfloat16),
            pltpu.VMEM((count, padded), jnp.bfloat16),
            pltpu.VMEM((2 * steps, rest, width), i16),
            pltpu.VMEM((2 * steps, rest, width), i16),
            pltpu.VMEM((steps, rest, width), i16),
            pltpu.VMEM((steps, rest, width), i16),
            pltpu.VMEM((steps - pieces, rest, width), i16),
            pltpu.VMEM((steps - pieces, rest, width), i16),
            pltpu.VMEM((12, part, block), i16),
            pltpu.VMEM((12, part, block), i16),
            pltpu.VMEM((8, part, block), i16),
            pltpu.VMEM((4, part, block), i16),
            pltpu.VMEM((2, part, block), i16),
            pltpu.VMEM((2, part, block), i16),
            pltpu.VMEM((part, block), i16),
            pltpu.VMEM((part, block), i16),
            pltpu.VMEM((2 * pieces, rest, width), jnp.float32),
            pltpu.VMEM((2 * pieces, rest, width), i16),
            pltpu.VMEM((pieces, rest, width), i16),
            dma((deep,)), dma,
            dma((nv - 1,)), dma((nv - 1,)),
            dma, dma((2 * steps,)),
            dma, dma((steps,)),
            dma, dma((steps - pieces,)),
            dma, dma((9,)),
            dma, dma,
            dma, dma((2,)),
            dma, dma,
            dma, dma((pieces,)),
        ],
        compiler_params=pltpu.CompilerParams(
            collective_id=0, has_side_effects=True, vmem_limit_bytes=60000 * 1024
        ),
    )(bold_series.reshape(length, columns // 128, 128), seed_index[None, :])
    return result


def solution(mesh):
    n, nv = mesh.shape["subj"], mesh.shape["vox"]
    in_specs = (P("subj", None, "vox"), P())
    out_specs = P(("vox", "subj"), None)
    return jax.shard_map(
        functools.partial(body, n, nv), mesh=mesh, in_specs=in_specs, out_specs=out_specs,
        check_vma=False,
    )
```

```python
import functools
import math

import jax
import jax.numpy as jnp
from jax import lax
from jax.experimental import pallas as pl
from jax.experimental.pallas import tpu as pltpu
from jax.sharding import PartitionSpec as P

clip_limit = 0.99
epsilon = 1e-05
MESH = pl.DeviceIdType.MESH
z_limit = 0.5 * math.log((1.0 + clip_limit) / (1.0 - clip_limit))
code_top = 32700.0
pieces = 2
ahead = 2
last = 4
late = 2
layers = 4
deep = 3
side_rows = 48


def encode(value, terms):
    scale = code_top / math.sqrt(terms * z_limit)
    root = value * lax.rsqrt(jnp.maximum(jnp.abs(value), 1e-30))
    return jnp.round(root * scale).astype(jnp.int32).astype(jnp.int16)


def decode(code, terms):
    scale = math.sqrt(terms * z_limit) / code_top
    root = code.astype(jnp.int32).astype(jnp.float32) * scale
    return root * jnp.abs(root)


def kernel(n, nv, chunk, side, bold, index, result, seeds, out, raw, norm, acc, pan_out, pan_in, pan_t,
           s1_out, s1_in, s2_out, s2_in, s3_out, s3_in, za_out, za_in, zb_out, zb_in,
           ta_out, ta_in, tb_out, tb_in, hold, x_out, x_in, series, pan_mate, held,
           load_sem, seed_sem, p_send, p_recv, a_send, a_recv, b_send, b_recv, c_send, c_recv,
           za_send, za_recv, zb_send, zb_recv, ta_send, ta_recv, tb_send, tb_recv, x_send, x_recv, e_send, e_recv):
    length, columns = norm.shape
    block = columns // n
    hi_count = n // 4
    steps = hi_count * pieces
    width = block // pieces
    main = pl.ds(side, seeds.shape[1] - side)
    far, cross = 2 * pieces, 2
    early = pieces if side else 0
    side_turn, side_next = 7, 9
    offsets = sorted(range(hi_count), key=lambda d: -min(d, hi_count - d))
    s = lax.axis_index("subj")
    v = lax.axis_index("vox")
    odd = lax.rem(v, 2)
    w1, w2 = 1 + odd, 2 - odd
    f, g = lax.rem(s // w1, 2), lax.rem(s // w2, 2)
    hi, lo = s // 4, lax.rem(s, 4)
    mate1 = s + w1 * (1 - 2 * f)
    mate2 = s + w2 * (1 - 2 * g)

    pair = hi // 2
    inner = lax.rem((hi + 1) // 2, 2)
    beside = hi + 1 - 2 * lax.rem(hi, 2)

    def target_of(step):
        turn = step // pieces
        order = [3 - 3 * pair, 2 - pair, beside, hi] if side else [
            lax.rem(hi + d, hi_count) for d in offsets
        ]
        layer = 0
        for place, h in enumerate(order):
            layer = layer + jnp.where(turn == place, h, 0)
        return layer

    loads, lines = columns // chunk, chunk // 128
    spin = target_of(0) * (4 * block // chunk) if side else 0

    def turned(i):
        return lax.rem(i + spin, loads)

    def load(i, j):
        line = turned(i) * lines + j
        return pltpu.make_async_copy(bold.at[:, line, :], raw.at[line], load_sem.at[lax.rem(i, deep)])

    fetch = pltpu.make_async_copy(index, seeds, seed_sem)
    fetch.start()
    def begin(i):
        for j in range(lines):
            load(i, j).start()

    for i in range(deep):
        begin(i)

    barrier = pltpu.get_barrier_semaphore()
    pl.semaphore_signal(barrier, inc=1, device_id={"subj": mate1}, device_id_type=MESH)
    pl.semaphore_signal(barrier, inc=1, device_id={"subj": mate2}, device_id_type=MESH)
    for j in range(1, hi_count):
        peer = lax.rem(hi + j, hi_count) * 4 + lo
        pl.semaphore_signal(barrier, inc=1, device_id={"subj": peer}, device_id_type=MESH)
    for j in range(1, nv):
        pl.semaphore_signal(
            barrier, inc=1, device_id={"vox": lax.rem(v + j, nv)}, device_id_type=MESH
        )

    acc[...] = jnp.zeros_like(acc)

    def arrive(i):
        whole = raw.at[pl.ds(turned(i) * lines, lines)]
        pltpu.make_async_copy(whole, whole, load_sem.at[lax.rem(i, deep)]).wait()

    def normalize(i):
        for j in range(lines):
            line = turned(i) * lines + j
            cols = pl.ds(pl.multiple_of(line * 128, 128), 128)
            x = raw[line]
            x = x - jnp.sum(x, axis=0, keepdims=True) * (1.0 / length)
            spread = jnp.sum(x * x, axis=0, keepdims=True) * (1.0 / length)
            norm[:, cols] = (x * lax.rsqrt(spread + epsilon)).astype(jnp.bfloat16)

    def pick(i):
        start = turned(i) * chunk
        cols = pl.ds(pl.multiple_of(start, 128), chunk)
        rows = lax.broadcasted_iota(jnp.int16, (chunk, seeds.shape[1]), 0)
        place = jnp.clip(seeds[...] - (v * columns + start), -1, chunk).astype(jnp.int16)
        hit = jnp.where(rows == place, jnp.bfloat16(1.0), jnp.bfloat16(0.0))
        acc[pl.ds(0, length), :] += jnp.dot(
            norm[:, cols], hit, preferred_element_type=jnp.float32,
        )

    def copy_series(j, gg):
        start = (target_of(0) * 4 + gg * w2 + (1 - f) * w1) * block
        return pltpu.make_async_remote_copy(
            src_ref=norm.at[:, pl.ds(pl.multiple_of(start, 128), block)], dst_ref=series.at[j],
            send_sem=e_send, recv_sem=e_recv.at[j], device_id={"subj": mate1},
            device_id_type=MESH,
        )

    def copy_panel():
        return pltpu.make_async_remote_copy(
            src_ref=pan_t.at[main], dst_ref=pan_mate, send_sem=e_send, recv_sem=e_recv.at[2],
            device_id={"subj": mate1}, device_id_type=MESH,
        )

    def meet():
        pl.semaphore_wait(barrier, 2 + (hi_count - 1) + (nv - 1))

    fetch.wait()
    arrive(0)
    begin(min(deep, loads - 1)) if deep < loads else None
    normalize(0)

    @pl.loop(1, loads)
    def _(i):
        if side:
            @pl.when(i == 2)
            def _():
                meet()
                copy_series(0, 1 - g).start()
                copy_series(1, g).start()

        arrive(i)

        @pl.when(i + deep < loads)
        def _():
            begin(i + deep)

        pick(i - 1)
        normalize(i)

    pick(loads - 1)

    if not side:
        meet()
    pan_out[...] = acc[pl.ds(0, length), :].astype(jnp.bfloat16)

    def panel_copy(j):
        return pltpu.make_async_remote_copy(
            src_ref=pan_out, dst_ref=pan_in.at[j - 1],
            send_sem=p_send.at[j - 1], recv_sem=p_recv.at[j - 1],
            device_id={"vox": lax.rem(v + j, nv)}, device_id_type=MESH,
        )

    for j in range(1, nv):
        panel_copy(j).start()
    for j in range(1, nv):
        panel_copy(j).wait_recv()
        acc[pl.ds(0, length), :] += pan_in[j - 1].astype(jnp.float32)
    pan_t[...] = acc[...].T.astype(jnp.bfloat16)
    if side:
        copy_panel().start()

    def transform(panel, voxels):
        cross = jnp.dot(panel, voxels, preferred_element_type=jnp.float32)
        c = jnp.clip(cross * (1.0 / length), -clip_limit, clip_limit)
        return 0.5 * (jnp.log(1.0 + c) - jnp.log(1.0 - c))

    def correlate(rows, cols):
        return transform(pan_t[rows, pl.ds(0, length)], norm[:, cols])

    def fisher_mate(step, j):
        cols = pl.ds(pl.multiple_of(lax.rem(step, pieces) * width, 128), width)
        return transform(pan_mate[:, pl.ds(0, length)], series[j, :, cols])

    def fisher(step, gg, ff):
        start = (target_of(step) * 4 + gg * w2 + ff * w1) * block
        start = start + lax.rem(step, pieces) * width
        return correlate(main, pl.ds(pl.multiple_of(start, 128), width))

    def copy1(k):
        return pltpu.make_async_remote_copy(
            src_ref=s1_out.at[k], dst_ref=s1_in.at[k], send_sem=a_send,
            recv_sem=a_recv.at[k], device_id={"subj": mate1}, device_id_type=MESH,
        )

    def copy2(k):
        return pltpu.make_async_remote_copy(
            src_ref=s2_out.at[k], dst_ref=s2_in.at[k], send_sem=b_send,
            recv_sem=b_recv.at[k], device_id={"subj": mate2}, device_id_type=MESH,
        )

    def copy3(k):
        target = target_of(k) * 4 + lo
        return pltpu.make_async_remote_copy(
            src_ref=s3_out.at[k], dst_ref=s3_in.at[k], send_sem=c_send,
            recv_sem=c_recv.at[k], device_id={"subj": target}, device_id_type=MESH,
        )

    def copy_z(k):
        return pltpu.make_async_remote_copy(
            src_ref=s3_out.at[k], dst_ref=s3_in.at[k], send_sem=c_send,
            recv_sem=c_recv.at[k], device_id={"subj": beside * 4 + lo}, device_id_type=MESH,
        )

    def copy_x(k):
        slot = lax.rem(k, pieces)
        return pltpu.make_async_remote_copy(
            src_ref=x_out.at[k], dst_ref=x_in.at[slot], send_sem=x_send,
            recv_sem=x_recv.at[slot], device_id={"subj": target_of(k) * 4 + lo},
            device_id_type=MESH,
        )

    def far_layer(e):
        return 3 - 3 * pair + (e // 4) * (2 * pair - 1)

    def side_fisher(layer, q):
        start = (layer * 4 + q) * block
        return correlate(pl.ds(0, side), pl.ds(pl.multiple_of(start, 128), block))

    def arrived(ref, sem):
        pltpu.make_async_remote_copy(
            src_ref=ref, dst_ref=ref, send_sem=tb_send, recv_sem=sem,
            device_id={"subj": mate1}, device_id_type=MESH,
        ).wait_recv()

    def copy_za(e):
        return pltpu.make_async_remote_copy(
            src_ref=za_out.at[e], dst_ref=za_in.at[e], send_sem=za_send,
            recv_sem=za_recv.at[jnp.minimum(e, 8)], device_id={"subj": beside * 4 + lo}, device_id_type=MESH,
        )

    def copy_zb(e):
        slot = lax.rem(e, 4)
        return pltpu.make_async_remote_copy(
            src_ref=zb_out.at[e], dst_ref=zb_in.at[slot], send_sem=zb_send,
            recv_sem=zb_recv, device_id={"subj": far_layer(e) * 4 + lo},
            device_id_type=MESH,
        )

    def copy_ta(k):
        return pltpu.make_async_remote_copy(
            src_ref=ta_out.at[k], dst_ref=ta_in.at[k], send_sem=ta_send,
            recv_sem=ta_recv.at[k], device_id={"subj": mate2}, device_id_type=MESH,
        )

    def copy_tb():
        return pltpu.make_async_remote_copy(
            src_ref=tb_out, dst_ref=tb_in, send_sem=tb_send,
            recv_sem=tb_recv, device_id={"subj": mate1}, device_id_type=MESH,
        )

    def layer_sum(gg, ff):
        q = gg * w2 + ff * w1
        return side_fisher(hi, q) + decode(za_in[q + 8], 1) + decode(zb_in[q], 2)

    @pl.loop(0, steps + last)
    def _(turn):
        @pl.when(turn < steps - early)
        def _():
            k = turn + early
            s1_out[2 * k] = encode(fisher(k, 1 - g, 1 - f), 1)
            copy1(2 * k).start()

        @pl.when((turn >= late) & (turn < steps - early + late))
        def _():
            k = turn + early - late
            s1_out[2 * k + 1] = encode(fisher(k, g, 1 - f), 1)
            copy1(2 * k + 1).start()

        if side:
            @pl.when(turn == side_next)
            def _():
                copy_ta(0).wait_recv()
                tb_out[...] = encode(layer_sum(g, 1 - f) + decode(ta_in[0], 4), 8)
                copy_tb().start()

        if side:
            @pl.when((turn < 2) & (inner == 0))
            def _():
                @pl.loop(4 * turn, 4 * turn + 4)
                def _(e):
                    za_out[e] = encode(side_fisher(far_layer(e), lax.rem(e, 4)), 1)
                    copy_za(e).start()

            @pl.when(turn == 2 - 2 * inner)
            def _():
                @pl.loop(0, 4)
                def _(q):
                    za_out[q + 8] = encode(side_fisher(beside, q), 1)
                    copy_za(q + 8).start()

        @pl.when((turn >= ahead) & (turn < steps + ahead))
        def _():
            k = turn - ahead
            mine = fisher(k, 1 - g, f)

            if side:
                @pl.when(k == 0)
                def _():
                    copy_series(0, 1 - g).wait_recv()
                    copy_panel().wait_recv()

                @pl.when(k < early)
                def _():
                    s2_out[k] = encode(mine + fisher_mate(k, 0), 2)

            @pl.when(k >= early)
            def _():
                copy1(2 * k).wait_recv()
                s2_out[k] = encode(mine + decode(s1_in[2 * k], 1), 2)

            copy2(k).start()

        if side:
            @pl.when((turn >= 2) & (turn < 5) & (inner == 1))
            def _():
                @pl.loop(2 * turn - 4, 2 * turn - 2 + 2 * (turn // 4))
                def _(e):
                    mine = side_fisher(far_layer(e), lax.rem(e, 4))
                    copy_za(e).wait_recv()
                    zb_out[e] = encode(mine + decode(za_in[e], 1), 2)
                    copy_zb(e).start()

            @pl.when(turn == side_turn)
            def _():
                arrived(za_in.at[pl.ds(8, 4)], za_recv.at[8])
                arrived(zb_in, zb_recv)
                ta_out[0] = encode(layer_sum(1 - g, 1 - f), 4)
                copy_ta(0).start()
                ta_out[1] = encode(layer_sum(1 - g, f), 4)
                copy_ta(1).start()

        @pl.when(turn >= last)
        def _():
            k = turn - last
            if side:
                @pl.when(k == 0)
                def _():
                    copy_series(1, g).wait_recv()

                @pl.when(k < early)
                def _():
                    held[...] = fisher(k, g, f) + fisher_mate(k, 1)

            @pl.when(k >= early)
            def _():
                mine = fisher(k, g, f)
                copy1(2 * k + 1).wait_recv()
                held[...] = mine + decode(s1_in[2 * k + 1], 1)

            mine = held[...]
            copy2(k).wait_recv()
            mine = mine + decode(s2_in[k], 2)

            if side:
                @pl.when((k < steps - pieces) & ((inner == 0) | (k >= far)))
                def _():
                    s3_out[k] = encode(mine, 4)
                    copy_z(k).start()

                @pl.when((k < far) & (inner == 1))
                def _():
                    hold[k] = mine
            else:
                @pl.when(k < steps - pieces)
                def _():
                    s3_out[k] = encode(mine, 4)
                    copy3(k).start()

            @pl.when(k >= steps - pieces)
            def _():
                p = k - steps + pieces
                cols = pl.ds(pl.multiple_of(p * width, 128), width)
                if side:
                    copy_z(far + p).wait_recv()
                    copy_x(p).wait_recv()
                    total = mine + decode(s3_in[far + p], 4) + decode(x_in[p], 8)
                    out[main, cols] = total * (1.0 / n)
                else:
                    out[main, cols] = mine

        if side:
            @pl.when((turn >= last + cross) & (turn < last + cross + far) & (inner == 1))
            def _():
                k = turn - last - cross
                copy_z(k).wait_recv()
                x_out[k] = encode(hold[k] + decode(s3_in[k], 4), 8)
                copy_x(k).start()

    if side:
        copy_ta(1).wait_recv()
        mine = layer_sum(g, f) + decode(ta_in[1], 4)
        copy_tb().wait_recv()
        out[pl.ds(0, side), :] = (mine + decode(tb_in[...], 8)) * (1.0 / n)
        result[...] = out[...].T
    else:
        for p in range(pieces):
            cols = pl.ds(p * width, width)
            total = out[main, cols]
            for k in range(p, steps - pieces, pieces):
                copy3(k).wait_recv()
                total = total + decode(s3_in[k], 4)
            out[main, cols] = total * (1.0 / n)
            result[cols, :] = out[:, cols].T

    for j in range(1, nv):
        panel_copy(j).wait_send()

    def sent(ref, sem):
        pltpu.make_async_remote_copy(
            src_ref=ref, dst_ref=ref, send_sem=sem, recv_sem=p_recv.at[0],
            device_id={"subj": mate1}, device_id_type=MESH,
        ).wait_send()

    sent(s1_out.at[pl.ds(2 * early, 2 * (steps - early))], a_send)
    sent(s2_out, b_send)
    if side:
        @pl.when(inner == 0)
        def _():
            sent(za_out, za_send)
            sent(s3_out, c_send)

        @pl.when(inner == 1)
        def _():
            sent(za_out.at[pl.ds(8, 4)], za_send)
            sent(s3_out.at[pl.ds(far, pieces)], c_send)
            sent(zb_out, zb_send)
            sent(x_out, x_send)

        sent(ta_out, ta_send)
        sent(tb_out, tb_send)
        sent(series, e_send)
        sent(pan_mate, e_send)
    else:
        sent(s3_out, c_send)


def body(n, nv, bold_series, seed_index):
    _, length, columns = bold_series.shape
    count = seed_index.shape[0]
    block = columns // n
    steps = n // 4 * pieces
    width = block // pieces
    padded = -(-length // 128) * 128
    chunk = 1024
    side = side_rows if n // 4 == layers else 0
    rest, part = count - side, max(side, 16)
    i16 = jnp.int16
    dma = pltpu.SemaphoreType.DMA
    result = pl.pallas_call(
        functools.partial(kernel, n, nv, chunk, side),
        out_shape=pltpu.VMEM((block, count), jnp.float32),
        in_specs=[pl.BlockSpec(memory_space=pltpu.HBM), pl.BlockSpec(memory_space=pltpu.HBM)],
        out_specs=pl.BlockSpec(memory_space=pltpu.VMEM),
        scratch_shapes=[
            pltpu.VMEM((1, count), jnp.int32),
            pltpu.VMEM((count, block), jnp.float32),
            pltpu.VMEM((columns // 128, length, 128), jnp.float32),
            pltpu.VMEM((length, columns), jnp.bfloat16),
            pltpu.VMEM((padded, count), jnp.float32),
            pltpu.VMEM((length, count), jnp.bfloat16),
            pltpu.VMEM((nv - 1, length, count), jnp.bfloat16),
            pltpu.VMEM((count, padded), jnp.bfloat16),
            pltpu.VMEM((2 * steps, rest, width), i16),
            pltpu.VMEM((2 * steps, rest, width), i16),
            pltpu.VMEM((steps, rest, width), i16),
            pltpu.VMEM((steps, rest, width), i16),
            pltpu.VMEM((steps - pieces, rest, width), i16),
            pltpu.VMEM((steps - pieces, rest, width), i16),
            pltpu.VMEM((12, part, block), i16),
            pltpu.VMEM((12, part, block), i16),
            pltpu.VMEM((8, part, block), i16),
            pltpu.VMEM((4, part, block), i16),
            pltpu.VMEM((2, part, block), i16),
            pltpu.VMEM((2, part, block), i16),
            pltpu.VMEM((part, block), i16),
            pltpu.VMEM((part, block), i16),
            pltpu.VMEM((2 * pieces, rest, width), jnp.float32),
            pltpu.VMEM((2 * pieces, rest, width), i16),
            pltpu.VMEM((pieces, rest, width), i16),
            pltpu.VMEM((2, length, block), jnp.bfloat16),
            pltpu.VMEM((rest, padded), jnp.bfloat16),
            pltpu.VMEM((rest, width), jnp.float32),
            dma((deep,)), dma,
            dma((nv - 1,)), dma((nv - 1,)),
            dma, dma((2 * steps,)),
            dma, dma((steps,)),
            dma, dma((steps - pieces,)),
            dma, dma((9,)),
            dma, dma,
            dma, dma((2,)),
            dma, dma,
            dma, dma((pieces,)),
            dma, dma((3,)),
        ],
        compiler_params=pltpu.CompilerParams(
            collective_id=0, has_side_effects=True, vmem_limit_bytes=60000 * 1024
        ),
    )(bold_series.reshape(length, columns // 128, 128), seed_index[None, :])
    return result


def solution(mesh):
    n, nv = mesh.shape["subj"], mesh.shape["vox"]
    in_specs = (P("subj", None, "vox"), P())
    out_specs = P(("vox", "subj"), None)
    return jax.shard_map(
        functools.partial(body, n, nv), mesh=mesh, in_specs=in_specs, out_specs=out_specs,
        check_vma=False,
    )
```

```python
import functools
import math

import jax
import jax.numpy as jnp
from jax import lax
from jax.experimental import pallas as pl
from jax.experimental.pallas import tpu as pltpu
from jax.sharding import PartitionSpec as P

clip_limit = 0.99
epsilon = 1e-05
MESH = pl.DeviceIdType.MESH
z_limit = 0.5 * math.log((1.0 + clip_limit) / (1.0 - clip_limit))
code_top = 32700.0
pieces = 2
ahead = 2
last = 4
late = 2
layers = 4
deep = 3
side_rows = 48


def encode(value, terms):
    scale = code_top / math.sqrt(terms * z_limit)
    root = value * lax.rsqrt(jnp.maximum(jnp.abs(value), 1e-30))
    return jnp.round(root * scale).astype(jnp.int32).astype(jnp.int16)


def decode(code, terms):
    scale = math.sqrt(terms * z_limit) / code_top
    root = code.astype(jnp.int32).astype(jnp.float32) * scale
    return root * jnp.abs(root)


def kernel(n, nv, chunk, side, bold, index, result, seeds, out, raw, norm, acc, pan_out, pan_in, pan_t,
           s1_out, s1_in, s2_out, s2_in, s3_out, s3_in, za_out, za_in, zb_out, zb_in,
           ta_out, ta_in, tb_out, tb_in, hold, x_out, x_in, series, pan_mate, held,
           load_sem, seed_sem, p_send, p_recv, a_send, a_recv, b_send, b_recv, c_send, c_recv,
           za_send, za_recv, zb_send, zb_recv, ta_send, ta_recv, tb_send, tb_recv, x_send, x_recv, e_send, e_recv):
    length, columns = norm.shape
    block = columns // n
    hi_count = n // 4
    steps = hi_count * pieces
    width = block // pieces
    main = pl.ds(side, seeds.shape[1] - side)
    far, cross = 2 * pieces, 2
    early = pieces if side else 0
    side_turn, side_next = 7, 9
    offsets = sorted(range(hi_count), key=lambda d: -min(d, hi_count - d))
    s = lax.axis_index("subj")
    v = lax.axis_index("vox")
    odd = lax.rem(v, 2)
    w1, w2 = 1 + odd, 2 - odd
    f, g = lax.rem(s // w1, 2), lax.rem(s // w2, 2)
    hi, lo = s // 4, lax.rem(s, 4)
    mate1 = s + w1 * (1 - 2 * f)
    mate2 = s + w2 * (1 - 2 * g)

    pair = hi // 2
    inner = lax.rem((hi + 1) // 2, 2)
    beside = hi + 1 - 2 * lax.rem(hi, 2)

    def target_of(step):
        turn = step // pieces
        order = [3 - 3 * pair, 2 - pair, beside, hi] if side else [
            lax.rem(hi + d, hi_count) for d in offsets
        ]
        layer = 0
        for place, h in enumerate(order):
            layer = layer + jnp.where(turn == place, h, 0)
        return layer

    loads, lines = columns // chunk, chunk // 128
    spin = target_of(0) * (4 * block // chunk) if side else 0

    ahead_half = odd * (1 - f) + (1 - odd) * (1 - g)

    def turned(i):
        place = jnp.where(i < 2, i + ahead_half * (1 - 2 * i), i) if side else i
        return lax.rem(place + spin, loads)

    def load(i, j):
        line = turned(i) * lines + j
        return pltpu.make_async_copy(bold.at[:, line, :], raw.at[line], load_sem.at[lax.rem(i, deep)])

    fetch = pltpu.make_async_copy(index, seeds, seed_sem)
    fetch.start()
    def begin(i):
        for j in range(lines):
            load(i, j).start()

    for i in range(deep - 1):
        begin(i)

    barrier = pltpu.get_barrier_semaphore()
    pl.semaphore_signal(barrier, inc=1, device_id={"subj": mate1}, device_id_type=MESH)
    pl.semaphore_signal(barrier, inc=1, device_id={"subj": mate2}, device_id_type=MESH)
    for j in range(1, hi_count):
        peer = lax.rem(hi + j, hi_count) * 4 + lo
        pl.semaphore_signal(barrier, inc=1, device_id={"subj": peer}, device_id_type=MESH)
    for j in range(1, nv):
        pl.semaphore_signal(
            barrier, inc=1, device_id={"vox": lax.rem(v + j, nv)}, device_id_type=MESH
        )

    acc[...] = jnp.zeros_like(acc)

    def arrive(i):
        whole = raw.at[pl.ds(turned(i) * lines, lines)]
        pltpu.make_async_copy(whole, whole, load_sem.at[lax.rem(i, deep)]).wait()

    def normalize(i):
        for j in range(lines):
            line = turned(i) * lines + j
            cols = pl.ds(pl.multiple_of(line * 128, 128), 128)
            x = raw[line]
            x = x - jnp.sum(x, axis=0, keepdims=True) * (1.0 / length)
            spread = jnp.sum(x * x, axis=0, keepdims=True) * (1.0 / length)
            norm[:, cols] = (x * lax.rsqrt(spread + epsilon)).astype(jnp.bfloat16)

    def pick(i):
        start = turned(i) * chunk
        cols = pl.ds(pl.multiple_of(start, 128), chunk)
        rows = lax.broadcasted_iota(jnp.int16, (chunk, seeds.shape[1]), 0)
        place = jnp.clip(seeds[...] - (v * columns + start), -1, chunk).astype(jnp.int16)
        hit = jnp.where(rows == place, jnp.bfloat16(1.0), jnp.bfloat16(0.0))
        acc[pl.ds(0, length), :] += jnp.dot(
            norm[:, cols], hit, preferred_element_type=jnp.float32,
        )

    def copy_series(j, gg):
        start = (target_of(0) * 4 + gg * w2 + (1 - f) * w1) * block
        return pltpu.make_async_remote_copy(
            src_ref=norm.at[:, pl.ds(pl.multiple_of(start, 128), block)], dst_ref=series.at[j],
            send_sem=e_send, recv_sem=e_recv.at[j], device_id={"subj": mate1},
            device_id_type=MESH,
        )

    def copy_panel():
        return pltpu.make_async_remote_copy(
            src_ref=pan_t.at[main], dst_ref=pan_mate, send_sem=e_send, recv_sem=e_recv.at[2],
            device_id={"subj": mate1}, device_id_type=MESH,
        )

    def meet():
        pl.semaphore_wait(barrier, 2 + (hi_count - 1) + (nv - 1))

    fetch.wait()
    arrive(0)
    for i in (deep - 1, deep):
        if i < loads:
            begin(i)
    normalize(0)

    @pl.loop(1, loads)
    def _(i):
        if side:
            @pl.when(i == 1)
            def _():
                meet()
                copy_series(0, 1 - g).start()

            @pl.when(i == 2)
            def _():
                copy_series(1, g).start()

        arrive(i)

        @pl.when(i + deep < loads)
        def _():
            begin(i + deep)

        pick(i - 1)
        normalize(i)

    pick(loads - 1)

    if not side:
        meet()
    pan_out[...] = acc[pl.ds(0, length), :].astype(jnp.bfloat16)

    def panel_copy(j):
        return pltpu.make_async_remote_copy(
            src_ref=pan_out, dst_ref=pan_in.at[j - 1],
            send_sem=p_send.at[j - 1], recv_sem=p_recv.at[j - 1],
            device_id={"vox": lax.rem(v + j, nv)}, device_id_type=MESH,
        )

    for j in range(1, nv):
        panel_copy(j).start()
    for j in range(1, nv):
        panel_copy(j).wait_recv()
        acc[pl.ds(0, length), :] += pan_in[j - 1].astype(jnp.float32)
    pan_t[...] = acc[...].T.astype(jnp.bfloat16)
    if side:
        copy_panel().start()

    def transform(panel, voxels):
        cross = jnp.dot(panel, voxels, preferred_element_type=jnp.float32)
        c = jnp.clip(cross * (1.0 / length), -clip_limit, clip_limit)
        return 0.5 * (jnp.log(1.0 + c) - jnp.log(1.0 - c))

    def correlate(rows, cols):
        return transform(pan_t[rows, pl.ds(0, length)], norm[:, cols])

    def fisher_mate(step, j):
        cols = pl.ds(pl.multiple_of(lax.rem(step, pieces) * width, 128), width)
        return transform(pan_mate[:, pl.ds(0, length)], series[j, :, cols])

    def fisher(step, gg, ff):
        start = (target_of(step) * 4 + gg * w2 + ff * w1) * block
        start = start + lax.rem(step, pieces) * width
        return correlate(main, pl.ds(pl.multiple_of(start, 128), width))

    def copy1(k):
        return pltpu.make_async_remote_copy(
            src_ref=s1_out.at[k], dst_ref=s1_in.at[k], send_sem=a_send,
            recv_sem=a_recv.at[k], device_id={"subj": mate1}, device_id_type=MESH,
        )

    def copy2(k):
        return pltpu.make_async_remote_copy(
            src_ref=s2_out.at[k], dst_ref=s2_in.at[k], send_sem=b_send,
            recv_sem=b_recv.at[k], device_id={"subj": mate2}, device_id_type=MESH,
        )

    def copy3(k):
        target = target_of(k) * 4 + lo
        return pltpu.make_async_remote_copy(
            src_ref=s3_out.at[k], dst_ref=s3_in.at[k], send_sem=c_send,
            recv_sem=c_recv.at[k], device_id={"subj": target}, device_id_type=MESH,
        )

    def copy_z(k):
        return pltpu.make_async_remote_copy(
            src_ref=s3_out.at[k], dst_ref=s3_in.at[k], send_sem=c_send,
            recv_sem=c_recv.at[k], device_id={"subj": beside * 4 + lo}, device_id_type=MESH,
        )

    def copy_x(k):
        slot = lax.rem(k, pieces)
        return pltpu.make_async_remote_copy(
            src_ref=x_out.at[k], dst_ref=x_in.at[slot], send_sem=x_send,
            recv_sem=x_recv.at[slot], device_id={"subj": target_of(k) * 4 + lo},
            device_id_type=MESH,
        )

    def far_layer(e):
        return 3 - 3 * pair + (e // 4) * (2 * pair - 1)

    def side_fisher(layer, q):
        start = (layer * 4 + q) * block
        return correlate(pl.ds(0, side), pl.ds(pl.multiple_of(start, 128), block))

    def arrived(ref, sem):
        pltpu.make_async_remote_copy(
            src_ref=ref, dst_ref=ref, send_sem=tb_send, recv_sem=sem,
            device_id={"subj": mate1}, device_id_type=MESH,
        ).wait_recv()

    def copy_za(e):
        return pltpu.make_async_remote_copy(
            src_ref=za_out.at[e], dst_ref=za_in.at[e], send_sem=za_send,
            recv_sem=za_recv.at[jnp.minimum(e, 8)], device_id={"subj": beside * 4 + lo}, device_id_type=MESH,
        )

    def copy_zb(e):
        slot = lax.rem(e, 4)
        return pltpu.make_async_remote_copy(
            src_ref=zb_out.at[e], dst_ref=zb_in.at[slot], send_sem=zb_send,
            recv_sem=zb_recv, device_id={"subj": far_layer(e) * 4 + lo},
            device_id_type=MESH,
        )

    def copy_ta(k):
        return pltpu.make_async_remote_copy(
            src_ref=ta_out.at[k], dst_ref=ta_in.at[k], send_sem=ta_send,
            recv_sem=ta_recv.at[k], device_id={"subj": mate2}, device_id_type=MESH,
        )

    def copy_tb():
        return pltpu.make_async_remote_copy(
            src_ref=tb_out, dst_ref=tb_in, send_sem=tb_send,
            recv_sem=tb_recv, device_id={"subj": mate1}, device_id_type=MESH,
        )

    def layer_sum(gg, ff):
        q = gg * w2 + ff * w1
        return side_fisher(hi, q) + decode(za_in[q + 8], 1) + decode(zb_in[q], 2)

    @pl.loop(0, steps + last)
    def _(turn):
        @pl.when(turn < steps - early)
        def _():
            k = turn + early
            s1_out[2 * k] = encode(fisher(k, 1 - g, 1 - f), 1)
            copy1(2 * k).start()

        @pl.when((turn >= late) & (turn < steps - early + late))
        def _():
            k = turn + early - late
            s1_out[2 * k + 1] = encode(fisher(k, g, 1 - f), 1)
            copy1(2 * k + 1).start()

        if side:
            @pl.when(turn == side_next)
            def _():
                copy_ta(0).wait_recv()
                tb_out[...] = encode(layer_sum(g, 1 - f) + decode(ta_in[0], 4), 8)
                copy_tb().start()

        if side:
            @pl.when((turn < 2) & (inner == 0))
            def _():
                @pl.loop(4 * turn, 4 * turn + 4)
                def _(e):
                    za_out[e] = encode(side_fisher(far_layer(e), lax.rem(e, 4)), 1)
                    copy_za(e).start()

            @pl.when(turn == 2 - 2 * inner)
            def _():
                @pl.loop(0, 4)
                def _(q):
                    za_out[q + 8] = encode(side_fisher(beside, q), 1)
                    copy_za(q + 8).start()

        @pl.when((turn >= ahead) & (turn < steps + ahead))
        def _():
            k = turn - ahead
            mine = fisher(k, 1 - g, f)

            if side:
                @pl.when(k == 0)
                def _():
                    copy_series(0, 1 - g).wait_recv()
                    copy_panel().wait_recv()

                @pl.when(k < early)
                def _():
                    s2_out[k] = encode(mine + fisher_mate(k, 0), 2)

            @pl.when(k >= early)
            def _():
                copy1(2 * k).wait_recv()
                s2_out[k] = encode(mine + decode(s1_in[2 * k], 1), 2)

            copy2(k).start()

        if side:
            @pl.when((turn >= 2) & (turn < 5) & (inner == 1))
            def _():
                @pl.loop(2 * turn - 4, 2 * turn - 2 + 2 * (turn // 4))
                def _(e):
                    mine = side_fisher(far_layer(e), lax.rem(e, 4))
                    copy_za(e).wait_recv()
                    zb_out[e] = encode(mine + decode(za_in[e], 1), 2)
                    copy_zb(e).start()

            @pl.when(turn == side_turn)
            def _():
                arrived(za_in.at[pl.ds(8, 4)], za_recv.at[8])
                arrived(zb_in, zb_recv)
                ta_out[0] = encode(layer_sum(1 - g, 1 - f), 4)
                copy_ta(0).start()
                ta_out[1] = encode(layer_sum(1 - g, f), 4)
                copy_ta(1).start()

        @pl.when(turn >= last)
        def _():
            k = turn - last
            if side:
                @pl.when(k == 0)
                def _():
                    copy_series(1, g).wait_recv()

                @pl.when(k < early)
                def _():
                    held[...] = fisher(k, g, f) + fisher_mate(k, 1)

            @pl.when(k >= early)
            def _():
                mine = fisher(k, g, f)
                copy1(2 * k + 1).wait_recv()
                held[...] = mine + decode(s1_in[2 * k + 1], 1)

            mine = held[...]
            copy2(k).wait_recv()
            mine = mine + decode(s2_in[k], 2)

            if side:
                @pl.when((k < steps - pieces) & ((inner == 0) | (k >= far)))
                def _():
                    s3_out[k] = encode(mine, 4)
                    copy_z(k).start()

                @pl.when((k < far) & (inner == 1))
                def _():
                    hold[k] = mine
            else:
                @pl.when(k < steps - pieces)
                def _():
                    s3_out[k] = encode(mine, 4)
                    copy3(k).start()

            @pl.when(k >= steps - pieces)
            def _():
                p = k - steps + pieces
                cols = pl.ds(pl.multiple_of(p * width, 128), width)
                if side:
                    copy_z(far + p).wait_recv()
                    copy_x(p).wait_recv()
                    total = mine + decode(s3_in[far + p], 4) + decode(x_in[p], 8)
                    out[main, cols] = total * (1.0 / n)
                else:
                    out[main, cols] = mine

        if side:
            @pl.when((turn >= last + cross) & (turn < last + cross + far) & (inner == 1))
            def _():
                k = turn - last - cross
                copy_z(k).wait_recv()
                x_out[k] = encode(hold[k] + decode(s3_in[k], 4), 8)
                copy_x(k).start()

    if side:
        copy_ta(1).wait_recv()
        mine = layer_sum(g, f) + decode(ta_in[1], 4)
        copy_tb().wait_recv()
        out[pl.ds(0, side), :] = (mine + decode(tb_in[...], 8)) * (1.0 / n)
        result[...] = out[...].T
    else:
        for p in range(pieces):
            cols = pl.ds(p * width, width)
            total = out[main, cols]
            for k in range(p, steps - pieces, pieces):
                copy3(k).wait_recv()
                total = total + decode(s3_in[k], 4)
            out[main, cols] = total * (1.0 / n)
            result[cols, :] = out[:, cols].T

    for j in range(1, nv):
        panel_copy(j).wait_send()

    def sent(ref, sem):
        pltpu.make_async_remote_copy(
            src_ref=ref, dst_ref=ref, send_sem=sem, recv_sem=p_recv.at[0],
            device_id={"subj": mate1}, device_id_type=MESH,
        ).wait_send()

    sent(s1_out.at[pl.ds(2 * early, 2 * (steps - early))], a_send)
    sent(s2_out, b_send)
    if side:
        @pl.when(inner == 0)
        def _():
            sent(za_out, za_send)
            sent(s3_out, c_send)

        @pl.when(inner == 1)
        def _():
            sent(za_out.at[pl.ds(8, 4)], za_send)
            sent(s3_out.at[pl.ds(far, pieces)], c_send)
            sent(zb_out, zb_send)
            sent(x_out, x_send)

        sent(ta_out, ta_send)
        sent(tb_out, tb_send)
        sent(series, e_send)
        sent(pan_mate, e_send)
    else:
        sent(s3_out, c_send)


def body(n, nv, bold_series, seed_index):
    _, length, columns = bold_series.shape
    count = seed_index.shape[0]
    block = columns // n
    steps = n // 4 * pieces
    width = block // pieces
    padded = -(-length // 128) * 128
    chunk = 1024
    side = side_rows if n // 4 == layers else 0
    rest, part = count - side, max(side, 16)
    i16 = jnp.int16
    dma = pltpu.SemaphoreType.DMA
    result = pl.pallas_call(
        functools.partial(kernel, n, nv, chunk, side),
        out_shape=pltpu.VMEM((block, count), jnp.float32),
        in_specs=[pl.BlockSpec(memory_space=pltpu.HBM), pl.BlockSpec(memory_space=pltpu.HBM)],
        out_specs=pl.BlockSpec(memory_space=pltpu.VMEM),
        scratch_shapes=[
            pltpu.VMEM((1, count), jnp.int32),
            pltpu.VMEM((count, block), jnp.float32),
            pltpu.VMEM((columns // 128, length, 128), jnp.float32),
            pltpu.VMEM((length, columns), jnp.bfloat16),
            pltpu.VMEM((padded, count), jnp.float32),
            pltpu.VMEM((length, count), jnp.bfloat16),
            pltpu.VMEM((nv - 1, length, count), jnp.bfloat16),
            pltpu.VMEM((count, padded), jnp.bfloat16),
            pltpu.VMEM((2 * steps, rest, width), i16),
            pltpu.VMEM((2 * steps, rest, width), i16),
            pltpu.VMEM((steps, rest, width), i16),
            pltpu.VMEM((steps, rest, width), i16),
            pltpu.VMEM((steps - pieces, rest, width), i16),
            pltpu.VMEM((steps - pieces, rest, width), i16),
            pltpu.VMEM((12, part, block), i16),
            pltpu.VMEM((12, part, block), i16),
            pltpu.VMEM((8, part, block), i16),
            pltpu.VMEM((4, part, block), i16),
            pltpu.VMEM((2, part, block), i16),
            pltpu.VMEM((2, part, block), i16),
            pltpu.VMEM((part, block), i16),
            pltpu.VMEM((part, block), i16),
            pltpu.VMEM((2 * pieces, rest, width), jnp.float32),
            pltpu.VMEM((2 * pieces, rest, width), i16),
            pltpu.VMEM((pieces, rest, width), i16),
            pltpu.VMEM((2, length, block), jnp.bfloat16),
            pltpu.VMEM((rest, padded), jnp.bfloat16),
            pltpu.VMEM((rest, width), jnp.float32),
            dma((deep,)), dma,
            dma((nv - 1,)), dma((nv - 1,)),
            dma, dma((2 * steps,)),
            dma, dma((steps,)),
            dma, dma((steps - pieces,)),
            dma, dma((9,)),
            dma, dma,
            dma, dma((2,)),
            dma, dma,
            dma, dma((pieces,)),
            dma, dma((3,)),
        ],
        compiler_params=pltpu.CompilerParams(
            collective_id=0, has_side_effects=True, vmem_limit_bytes=60000 * 1024
        ),
    )(bold_series.reshape(length, columns // 128, 128), seed_index[None, :])
    return result


def solution(mesh):
    n, nv = mesh.shape["subj"], mesh.shape["vox"]
    in_specs = (P("subj", None, "vox"), P())
    out_specs = P(("vox", "subj"), None)
    return jax.shard_map(
        functools.partial(body, n, nv), mesh=mesh, in_specs=in_specs, out_specs=out_specs,
        check_vma=False,
    )
```

```python
import functools
import math

import jax
import jax.numpy as jnp
from jax import lax
from jax.experimental import pallas as pl
from jax.experimental.pallas import tpu as pltpu
from jax.sharding import PartitionSpec as P

clip_limit = 0.99
epsilon = 1e-05
MESH = pl.DeviceIdType.MESH
z_limit = 0.5 * math.log((1.0 + clip_limit) / (1.0 - clip_limit))
code_top = 32700.0
pieces = 2
ahead = 2
last = 4
late = 2
layers = 4
deep = 3
side_rows = 48


def encode(value, terms):
    scale = code_top / math.sqrt(terms * z_limit)
    root = value * lax.rsqrt(jnp.maximum(jnp.abs(value), 1e-30))
    return jnp.round(root * scale).astype(jnp.int32).astype(jnp.int16)


def decode(code, terms):
    scale = math.sqrt(terms * z_limit) / code_top
    root = code.astype(jnp.int32).astype(jnp.float32) * scale
    return root * jnp.abs(root)


def kernel(n, nv, chunk, side, bold, index, result, seeds, out, raw, norm, acc, pan_out, pan_in, pan_t,
           s1_out, s1_in, s2_out, s2_in, s3_out, s3_in, za_out, za_in, zb_out, zb_in,
           ta_out, ta_in, tb_out, tb_in, hold, x_out, x_in, series, pan_mate, held,
           load_sem, seed_sem, p_send, p_recv, a_send, a_recv, b_send, b_recv, c_send, c_recv,
           za_send, za_recv, zb_send, zb_recv, ta_send, ta_recv, tb_send, tb_recv, x_send, x_recv, e_send, e_recv):
    length, columns = norm.shape
    block = columns // n
    hi_count = n // 4
    steps = hi_count * pieces
    width = block // pieces
    count = seeds.shape[1]
    main = pl.ds(side, seeds.shape[1] - side)
    far, cross = 2 * pieces, 2
    early = pieces if side else 0
    side_turn, side_next = 7, 9
    offsets = sorted(range(hi_count), key=lambda d: -min(d, hi_count - d))
    s = lax.axis_index("subj")
    v = lax.axis_index("vox")
    odd = lax.rem(v, 2)
    w1, w2 = 1 + odd, 2 - odd
    f, g = lax.rem(s // w1, 2), lax.rem(s // w2, 2)
    hi, lo = s // 4, lax.rem(s, 4)
    mate1 = s + w1 * (1 - 2 * f)
    mate2 = s + w2 * (1 - 2 * g)

    pair = hi // 2
    inner = lax.rem((hi + 1) // 2, 2)
    beside = hi + 1 - 2 * lax.rem(hi, 2)

    def target_of(step):
        turn = step // pieces
        order = [3 - 3 * pair, 2 - pair, beside, hi] if side else [
            lax.rem(hi + d, hi_count) for d in offsets
        ]
        layer = 0
        for place, h in enumerate(order):
            layer = layer + jnp.where(turn == place, h, 0)
        return layer

    loads, lines = columns // chunk, chunk // 128
    spin = target_of(0) * (4 * block // chunk) if side else 0

    ahead_half = odd * (1 - f) + (1 - odd) * (1 - g)

    def turned(i):
        place = jnp.where(i < 2, i + ahead_half * (1 - 2 * i), i) if side else i
        return lax.rem(place + spin, loads)

    def load(i, j):
        line = turned(i) * lines + j
        return pltpu.make_async_copy(bold.at[:, line, :], raw.at[line], load_sem.at[lax.rem(i, deep)])

    fetch = pltpu.make_async_copy(index, seeds, seed_sem)
    fetch.start()
    def begin(i):
        for j in range(lines):
            load(i, j).start()

    for i in range(deep - 1):
        begin(i)

    barrier = pltpu.get_barrier_semaphore()
    pl.semaphore_signal(barrier, inc=1, device_id={"subj": mate1}, device_id_type=MESH)
    pl.semaphore_signal(barrier, inc=1, device_id={"subj": mate2}, device_id_type=MESH)
    if side:
        for peer in (beside, inner * (3 - hi) + (1 - inner) * (2 - pair)):
            pl.semaphore_signal(
                barrier, inc=1, device_id={"subj": peer * 4 + lo}, device_id_type=MESH
            )
    else:
        for j in range(1, hi_count):
            peer = lax.rem(hi + j, hi_count) * 4 + lo
            pl.semaphore_signal(barrier, inc=1, device_id={"subj": peer}, device_id_type=MESH)
    for j in range(1, nv):
        pl.semaphore_signal(
            barrier, inc=1, device_id={"vox": lax.rem(v + j, nv)}, device_id_type=MESH
        )

    acc[...] = jnp.zeros_like(acc)

    def arrive(i):
        whole = raw.at[pl.ds(turned(i) * lines, lines)]
        pltpu.make_async_copy(whole, whole, load_sem.at[lax.rem(i, deep)]).wait()

    def normalize(i):
        for j in range(lines):
            line = turned(i) * lines + j
            cols = pl.ds(pl.multiple_of(line * 128, 128), 128)
            x = raw[line]
            x = x - jnp.sum(x, axis=0, keepdims=True) * (1.0 / length)
            spread = jnp.sum(x * x, axis=0, keepdims=True) * (1.0 / length)
            norm[:, cols] = (x * lax.rsqrt(spread + epsilon)).astype(jnp.bfloat16)

    def pick(i):
        start = turned(i) * chunk
        cols = pl.ds(pl.multiple_of(start, 128), chunk)
        rows = lax.broadcasted_iota(jnp.int16, (chunk, seeds.shape[1]), 0)
        place = jnp.clip(seeds[...] - (v * columns + start), -1, chunk).astype(jnp.int16)
        hit = jnp.where(rows == place, jnp.bfloat16(1.0), jnp.bfloat16(0.0))
        acc[pl.ds(0, length), :] += jnp.dot(
            norm[:, cols], hit, preferred_element_type=jnp.float32,
        )

    def copy_series(j, gg):
        start = (target_of(0) * 4 + gg * w2 + (1 - f) * w1) * block
        return pltpu.make_async_remote_copy(
            src_ref=norm.at[:, pl.ds(pl.multiple_of(start, 128), block)], dst_ref=series.at[j],
            send_sem=e_send, recv_sem=e_recv.at[j], device_id={"subj": mate1},
            device_id_type=MESH,
        )

    def copy_panel():
        return pltpu.make_async_remote_copy(
            src_ref=pan_t.at[main], dst_ref=pan_mate, send_sem=e_send, recv_sem=e_recv.at[2],
            device_id={"subj": mate1}, device_id_type=MESH,
        )

    def meet():
        along = 1 + 2 * inner if side else hi_count - 1
        pl.semaphore_wait(barrier, 2 + along + (nv - 1))

    fetch.wait()
    arrive(0)
    for i in (deep - 1, deep):
        if i < loads:
            begin(i)
    normalize(0)

    @pl.loop(1, loads)
    def _(i):
        if side:
            @pl.when(i == 1)
            def _():
                meet()
                copy_series(0, 1 - g).start()

            @pl.when(i == 2)
            def _():
                copy_series(1, g).start()

        arrive(i)

        @pl.when(i + deep < loads)
        def _():
            begin(i + deep)

        pick(i - 1)
        normalize(i)

    pick(loads - 1)

    if not side:
        meet()
    pan_out[...] = acc[pl.ds(0, length), :].astype(jnp.bfloat16)

    def panel_copy(j):
        return pltpu.make_async_remote_copy(
            src_ref=pan_out, dst_ref=pan_in.at[j - 1],
            send_sem=p_send.at[j - 1], recv_sem=p_recv.at[j - 1],
            device_id={"vox": lax.rem(v + j, nv)}, device_id_type=MESH,
        )

    for j in range(1, nv):
        panel_copy(j).start()
    for j in range(1, nv):
        panel_copy(j).wait_recv()
        acc[pl.ds(0, length), :] += pan_in[j - 1].astype(jnp.float32)
    pan_t[...] = acc[...].T.astype(jnp.bfloat16)
    if side:
        copy_panel().start()

    def transform(panel, voxels):
        cross = jnp.dot(panel, voxels, preferred_element_type=jnp.float32)
        c = jnp.clip(cross * (1.0 / length), -clip_limit, clip_limit)
        return 0.5 * (jnp.log(1.0 + c) - jnp.log(1.0 - c))

    def correlate(rows, cols):
        return transform(pan_t[rows, pl.ds(0, length)], norm[:, cols])

    def fisher_mate(step, j):
        cols = pl.ds(pl.multiple_of(lax.rem(step, pieces) * width, 128), width)
        return transform(pan_mate[:, pl.ds(0, length)], series[j, :, cols])

    def fisher(step, gg, ff):
        start = (target_of(step) * 4 + gg * w2 + ff * w1) * block
        start = start + lax.rem(step, pieces) * width
        return correlate(main, pl.ds(pl.multiple_of(start, 128), width))

    def copy1(k):
        return pltpu.make_async_remote_copy(
            src_ref=s1_out.at[k], dst_ref=s1_in.at[k], send_sem=a_send,
            recv_sem=a_recv.at[k], device_id={"subj": mate1}, device_id_type=MESH,
        )

    def copy2(k):
        return pltpu.make_async_remote_copy(
            src_ref=s2_out.at[k], dst_ref=s2_in.at[k], send_sem=b_send,
            recv_sem=b_recv.at[k], device_id={"subj": mate2}, device_id_type=MESH,
        )

    def copy3(k):
        target = target_of(k) * 4 + lo
        return pltpu.make_async_remote_copy(
            src_ref=s3_out.at[k], dst_ref=s3_in.at[k], send_sem=c_send,
            recv_sem=c_recv.at[k], device_id={"subj": target}, device_id_type=MESH,
        )

    def copy_z(k):
        return pltpu.make_async_remote_copy(
            src_ref=s3_out.at[k], dst_ref=s3_in.at[k], send_sem=c_send,
            recv_sem=c_recv.at[k], device_id={"subj": beside * 4 + lo}, device_id_type=MESH,
        )

    def copy_x(k):
        slot = lax.rem(k, pieces)
        return pltpu.make_async_remote_copy(
            src_ref=x_out.at[k], dst_ref=x_in.at[slot], send_sem=x_send,
            recv_sem=x_recv.at[slot], device_id={"subj": target_of(k) * 4 + lo},
            device_id_type=MESH,
        )

    def far_layer(e):
        return 3 - 3 * pair + (e // 4) * (2 * pair - 1)

    def side_fisher(layer, q):
        start = (layer * 4 + q) * block
        return correlate(pl.ds(0, side), pl.ds(pl.multiple_of(start, 128), block))

    def arrived(ref, sem):
        pltpu.make_async_remote_copy(
            src_ref=ref, dst_ref=ref, send_sem=tb_send, recv_sem=sem,
            device_id={"subj": mate1}, device_id_type=MESH,
        ).wait_recv()

    def copy_za(e):
        return pltpu.make_async_remote_copy(
            src_ref=za_out.at[e], dst_ref=za_in.at[e], send_sem=za_send,
            recv_sem=za_recv.at[jnp.minimum(e, 8)], device_id={"subj": beside * 4 + lo}, device_id_type=MESH,
        )

    def copy_zb(e):
        slot = lax.rem(e, 4)
        return pltpu.make_async_remote_copy(
            src_ref=zb_out.at[e], dst_ref=zb_in.at[slot], send_sem=zb_send,
            recv_sem=zb_recv, device_id={"subj": far_layer(e) * 4 + lo},
            device_id_type=MESH,
        )

    def copy_ta(k):
        return pltpu.make_async_remote_copy(
            src_ref=ta_out.at[k], dst_ref=ta_in.at[k], send_sem=ta_send,
            recv_sem=ta_recv.at[k], device_id={"subj": mate2}, device_id_type=MESH,
        )

    def copy_tb():
        return pltpu.make_async_remote_copy(
            src_ref=tb_out, dst_ref=tb_in, send_sem=tb_send,
            recv_sem=tb_recv, device_id={"subj": mate1}, device_id_type=MESH,
        )

    def layer_sum(gg, ff):
        q = gg * w2 + ff * w1
        return side_fisher(hi, q) + decode(za_in[q + 8], 1) + decode(zb_in[q], 2)

    @pl.loop(0, steps + last)
    def _(turn):
        @pl.when(turn < steps - early)
        def _():
            k = turn + early
            s1_out[2 * k] = encode(fisher(k, 1 - g, 1 - f), 1)
            copy1(2 * k).start()

        @pl.when((turn >= late) & (turn < steps - early + late))
        def _():
            k = turn + early - late
            s1_out[2 * k + 1] = encode(fisher(k, g, 1 - f), 1)
            copy1(2 * k + 1).start()

        if side:
            @pl.when(turn == side_next)
            def _():
                copy_ta(0).wait_recv()
                tb_out[...] = encode(layer_sum(g, 1 - f) + decode(ta_in[0], 4), 8)
                copy_tb().start()

        if side:
            @pl.when((turn < 2) & (inner == 0))
            def _():
                @pl.loop(4 * turn, 4 * turn + 4)
                def _(e):
                    za_out[e] = encode(side_fisher(far_layer(e), lax.rem(e, 4)), 1)
                    copy_za(e).start()

            @pl.when(turn == 2 - 2 * inner)
            def _():
                @pl.loop(0, 4)
                def _(q):
                    za_out[q + 8] = encode(side_fisher(beside, q), 1)
                    copy_za(q + 8).start()

        @pl.when((turn >= ahead) & (turn < steps + ahead))
        def _():
            k = turn - ahead
            mine = fisher(k, 1 - g, f)

            if side:
                @pl.when(k == 0)
                def _():
                    copy_series(0, 1 - g).wait_recv()
                    copy_panel().wait_recv()

                @pl.when(k < early)
                def _():
                    s2_out[k] = encode(mine + fisher_mate(k, 0), 2)

            @pl.when(k >= early)
            def _():
                copy1(2 * k).wait_recv()
                s2_out[k] = encode(mine + decode(s1_in[2 * k], 1), 2)

            copy2(k).start()

        if side:
            @pl.when((turn >= 2) & (turn < 5) & (inner == 1))
            def _():
                @pl.loop(2 * turn - 4, 2 * turn - 2 + 2 * (turn // 4))
                def _(e):
                    mine = side_fisher(far_layer(e), lax.rem(e, 4))
                    copy_za(e).wait_recv()
                    zb_out[e] = encode(mine + decode(za_in[e], 1), 2)
                    copy_zb(e).start()

            @pl.when(turn == side_turn)
            def _():
                arrived(za_in.at[pl.ds(8, 4)], za_recv.at[8])
                arrived(zb_in, zb_recv)
                ta_out[0] = encode(layer_sum(1 - g, 1 - f), 4)
                copy_ta(0).start()
                ta_out[1] = encode(layer_sum(1 - g, f), 4)
                copy_ta(1).start()

        @pl.when(turn >= last)
        def _():
            k = turn - last
            if side:
                @pl.when(k == 0)
                def _():
                    copy_series(1, g).wait_recv()

                @pl.when(k < early)
                def _():
                    held[...] = fisher(k, g, f) + fisher_mate(k, 1)

            @pl.when(k >= early)
            def _():
                mine = fisher(k, g, f)
                copy1(2 * k + 1).wait_recv()
                held[...] = mine + decode(s1_in[2 * k + 1], 1)

            mine = held[...]
            copy2(k).wait_recv()
            mine = mine + decode(s2_in[k], 2)

            if side:
                @pl.when((k < steps - pieces) & ((inner == 0) | (k >= far)))
                def _():
                    s3_out[k] = encode(mine, 4)
                    copy_z(k).start()

                @pl.when((k < far) & (inner == 1))
                def _():
                    hold[k] = mine
            else:
                @pl.when(k < steps - pieces)
                def _():
                    s3_out[k] = encode(mine, 4)
                    copy3(k).start()

            @pl.when(k >= steps - pieces)
            def _():
                p = k - steps + pieces
                cols = pl.ds(pl.multiple_of(p * width, 128), width)
                if side:
                    copy_z(far + p).wait_recv()
                    copy_x(p).wait_recv()
                    total = mine + decode(s3_in[far + p], 4) + decode(x_in[p], 8)
                    out[main, cols] = total * (1.0 / n)
                    result[cols, pl.ds(128, count - 128)] = out[pl.ds(128, count - 128), cols].T
                else:
                    out[main, cols] = mine

        if side:
            @pl.when((turn >= last + cross) & (turn < last + cross + far) & (inner == 1))
            def _():
                k = turn - last - cross
                copy_z(k).wait_recv()
                x_out[k] = encode(hold[k] + decode(s3_in[k], 4), 8)
                copy_x(k).start()

    if side:
        copy_ta(1).wait_recv()
        mine = layer_sum(g, f) + decode(ta_in[1], 4)
        copy_tb().wait_recv()
        out[pl.ds(0, side), :] = (mine + decode(tb_in[...], 8)) * (1.0 / n)
        result[:, pl.ds(0, 128)] = out[pl.ds(0, 128), :].T
    else:
        for p in range(pieces):
            cols = pl.ds(p * width, width)
            total = out[main, cols]
            for k in range(p, steps - pieces, pieces):
                copy3(k).wait_recv()
                total = total + decode(s3_in[k], 4)
            out[main, cols] = total * (1.0 / n)
            result[cols, :] = out[:, cols].T

    for j in range(1, nv):
        panel_copy(j).wait_send()

    def sent(ref, sem):
        pltpu.make_async_remote_copy(
            src_ref=ref, dst_ref=ref, send_sem=sem, recv_sem=p_recv.at[0],
            device_id={"subj": mate1}, device_id_type=MESH,
        ).wait_send()

    sent(s1_out.at[pl.ds(2 * early, 2 * (steps - early))], a_send)
    sent(s2_out, b_send)
    if side:
        @pl.when(inner == 0)
        def _():
            sent(za_out, za_send)
            sent(s3_out, c_send)

        @pl.when(inner == 1)
        def _():
            sent(za_out.at[pl.ds(8, 4)], za_send)
            sent(s3_out.at[pl.ds(far, pieces)], c_send)
            sent(zb_out, zb_send)
            sent(x_out, x_send)

        sent(ta_out, ta_send)
        sent(tb_out, tb_send)
        sent(series, e_send)
        sent(pan_mate, e_send)
    else:
        sent(s3_out, c_send)


def body(n, nv, bold_series, seed_index):
    _, length, columns = bold_series.shape
    count = seed_index.shape[0]
    block = columns // n
    steps = n // 4 * pieces
    width = block // pieces
    padded = -(-length // 128) * 128
    chunk = 1024
    side = side_rows if n // 4 == layers else 0
    rest, part = count - side, max(side, 16)
    i16 = jnp.int16
    dma = pltpu.SemaphoreType.DMA
    result = pl.pallas_call(
        functools.partial(kernel, n, nv, chunk, side),
        out_shape=pltpu.VMEM((block, count), jnp.float32),
        in_specs=[pl.BlockSpec(memory_space=pltpu.HBM), pl.BlockSpec(memory_space=pltpu.HBM)],
        out_specs=pl.BlockSpec(memory_space=pltpu.VMEM),
        scratch_shapes=[
            pltpu.VMEM((1, count), jnp.int32),
            pltpu.VMEM((count, block), jnp.float32),
            pltpu.VMEM((columns // 128, length, 128), jnp.float32),
            pltpu.VMEM((length, columns), jnp.bfloat16),
            pltpu.VMEM((padded, count), jnp.float32),
            pltpu.VMEM((length, count), jnp.bfloat16),
            pltpu.VMEM((nv - 1, length, count), jnp.bfloat16),
            pltpu.VMEM((count, padded), jnp.bfloat16),
            pltpu.VMEM((2 * steps, rest, width), i16),
            pltpu.VMEM((2 * steps, rest, width), i16),
            pltpu.VMEM((steps, rest, width), i16),
            pltpu.VMEM((steps, rest, width), i16),
            pltpu.VMEM((steps - pieces, rest, width), i16),
            pltpu.VMEM((steps - pieces, rest, width), i16),
            pltpu.VMEM((12, part, block), i16),
            pltpu.VMEM((12, part, block), i16),
            pltpu.VMEM((8, part, block), i16),
            pltpu.VMEM((4, part, block), i16),
            pltpu.VMEM((2, part, block), i16),
            pltpu.VMEM((2, part, block), i16),
            pltpu.VMEM((part, block), i16),
            pltpu.VMEM((part, block), i16),
            pltpu.VMEM((2 * pieces, rest, width), jnp.float32),
            pltpu.VMEM((2 * pieces, rest, width), i16),
            pltpu.VMEM((pieces, rest, width), i16),
            pltpu.VMEM((2, length, block), jnp.bfloat16),
            pltpu.VMEM((rest, padded), jnp.bfloat16),
            pltpu.VMEM((rest, width), jnp.float32),
            dma((deep,)), dma,
            dma((nv - 1,)), dma((nv - 1,)),
            dma, dma((2 * steps,)),
            dma, dma((steps,)),
            dma, dma((steps - pieces,)),
            dma, dma((9,)),
            dma, dma,
            dma, dma((2,)),
            dma, dma,
            dma, dma((pieces,)),
            dma, dma((3,)),
        ],
        compiler_params=pltpu.CompilerParams(
            collective_id=0, has_side_effects=True, vmem_limit_bytes=60000 * 1024
        ),
    )(bold_series.reshape(length, columns // 128, 128), seed_index[None, :])
    return result


def solution(mesh):
    n, nv = mesh.shape["subj"], mesh.shape["vox"]
    in_specs = (P("subj", None, "vox"), P())
    out_specs = P(("vox", "subj"), None)
    return jax.shard_map(
        functools.partial(body, n, nv), mesh=mesh, in_specs=in_specs, out_specs=out_specs,
        check_vma=False,
    )
```
